32 devices in a mesh: gx: 8 (over z, x), gy: 4 (over y, core).
Axes of the slice: x: 2, y: 2, z: 4, core: 2. Of those that a mesh axis runs over, the one named last changes fastest.
Arguments:
- vectors: float32 [8, 2, 2, 128, 1024], P(None, None, None, 'gx', 'gy'), may hold values from -6 to 6
- bonds: float32 [3, 128, 1024], P(None, 'gx', 'gy'), may hold values from 0.5 to 1.5
- onsite: float32 [2, 128, 1024], P(None, 'gx', 'gy'), may hold values from -1 to 1
Outputs:
- moment_rows: float32 [2, 3, 3, 128], P(None, None, None, 'gx')
- left_last: bfloat16 [8, 2, 2, 128, 1024], P(None, None, None, 'gx', 'gy')
- right_last: bfloat16 [8, 2, 2, 128, 1024], P(None, None, None, 'gx', 'gy')
The draws below stay inside these ranges and needn't reach their ends.
All inputs are finite; a program needn't handle non-finite values.
Results may differ from the reference program's by a relative error of at most 0.001.
Values sent between devices are 32-bit elements; how exact they have to be, the bound alone decides.
A program may use at most 64 MiB of HBM per device.

```python
import math
import jax
import jax.numpy as jnp

VECTORS = 8
MOMENTS = 3
NX = 128
NY = 1024


def block_scale(stream_key, shape, shards, low, top_value):
    def one(position, blocks):
        draws = jax.random.uniform(jax.random.fold_in(jax.random.fold_in(stream_key, 6), position), (blocks,), jnp.float32, low / len(shards), top_value / len(shards))
        return jnp.repeat(jnp.exp(draws), shape[position] // blocks).reshape((-1,) + (1,) * (len(shape) - position - 1))

    gain = one(*shards[0])
    for cut in shards[1:]:
        gain = gain * one(*cut)
    return gain


def scatter_about(stream_key, dims, scale, limit, split=(), dtype=jnp.bfloat16):
    gain = block_scale(stream_key, dims, split, -0.22, 0.18) if split else 1.0
    array = jax.random.normal(stream_key, dims, jnp.float32) * scale * gain
    return jnp.minimum(jnp.maximum(array, -limit), limit).astype(dtype)


def setup_inputs(seed: int = 0) -> dict:
    seeds = jax.random.split(jax.random.key(seed), 4)
    vectors = scatter_about(seeds[0], (VECTORS, 2, 2, NX, NY), 1.0, 6.0, ((3, 8), (4, 4)), jnp.float32)
    bonds = jnp.clip(jnp.exp(math.log(1.5) - 1.0986123 * jax.random.uniform(seeds[1], (3, NX, NY), jnp.float32) ** block_scale(seeds[1], (3, NX, NY), ((1, 8), (2, 4)), -0.2, 0.2)), 0.5, 1.5)
    onsite = jnp.clip(jax.random.uniform(seeds[2], (2, NX, NY), jnp.float32, -1.0, 1.0) * block_scale(seeds[2], (2, NX, NY), ((1, 8), (2, 4)), -0.4, 0.0), -1.0, 1.0)
    return {"vectors": vectors, "bonds": bonds, "onsite": onsite}


SCALE = 6.0
OFFSETS = (1.0, -0.5, -0.5)
UNITS = (1.0, 1.0, 1.0)


def bond_sums(vector_field, bonds, weights):
    site_a = vector_field[:, :, 0]
    site_b = vector_field[:, :, 1]
    raised_one = jnp.roll(bonds[1], -1, 0)
    raised_two = jnp.roll(bonds[2], -1, 1)
    into_a = (weights[0] * bonds[0] * site_b
              + weights[1] * bonds[1] * jnp.roll(site_b, 1, 2)
              + weights[2] * bonds[2] * jnp.roll(site_b, 1, 3))
    into_b = (weights[0] * bonds[0] * site_a
              + weights[1] * raised_one * jnp.roll(site_a, -1, 2)
              + weights[2] * raised_two * jnp.roll(site_a, -1, 3))
    return site_a, site_b, into_a, into_b


def hamilton(vector_field, bonds, onsite):
    site_a, site_b, into_a, into_b = bond_sums(vector_field, bonds, UNITS)
    return jnp.stack([(onsite[0] * site_a + into_a) / SCALE,
                      (onsite[1] * site_b + into_b) / SCALE], axis=2)


def velocity(vector_field, bonds):
    site_a, site_b, sum_a, sum_b = bond_sums(vector_field, bonds, OFFSETS)
    image_a = jnp.stack([sum_a[:, 1], -sum_a[:, 0]], axis=1)
    image_b = jnp.stack([-sum_b[:, 1], sum_b[:, 0]], axis=1)
    return jnp.stack([image_a, image_b], axis=2)


def intersection(left, right):
    real_rows = jnp.sum(left[:, 0] * right[:, 0] + left[:, 1] * right[:, 1], axis=(0, 1, 3))
    imag_rows = jnp.sum(left[:, 0] * right[:, 1] - left[:, 1] * right[:, 0], axis=(0, 1, 3))
    return jnp.stack([real_rows, imag_rows])


def reference(vectors, bonds, onsite):
    right_chain = [vectors]
    for level in range(1, MOMENTS):
        stepped = hamilton(right_chain[level - 1], bonds, onsite)
        right_chain.append(stepped if level == 1 else 2.0 * stepped - right_chain[level - 2])
    rights = [velocity(entry, bonds) for entry in right_chain]
    lefts = [rights[0]]
    for level in range(1, MOMENTS):
        stepped = hamilton(lefts[level - 1], bonds, onsite)
        lefts.append(stepped if level == 1 else 2.0 * stepped - lefts[level - 2])
    moments = jnp.stack([jnp.stack([intersection(lefts[order], rights[other]) for other in range(MOMENTS)], axis=1)
                         for order in range(MOMENTS)], axis=1)
    moments = moments / float(VECTORS * NY)
    return moments, lefts[-1].astype(jnp.bfloat16), rights[-1].astype(jnp.bfloat16)
```

```python
import functools
import jax
import jax.numpy as jnp
from jax import lax
from jax.experimental import pallas as pl
from jax.experimental.pallas import tpu as pltpu
from jax.sharding import PartitionSpec as P

MOMENTS = 3
SCALE = 6.0
EDGE = 2
GROUP = 4
HALF = 64
LANES = 128
GRANT = 16 * 1024 * 1024
MESH = pl.DeviceIdType.MESH


def bond_terms(a, b, fields, left, right, up, down):
    b0, b1, b2, b1d, b2r = fields
    return b0 * b, b1 * up(b) + b2 * left(b), b0 * a, b1d * down(a) + b2r * right(a)


def kernel(
    gxn, gyn, vec, bonds, onsite, out_mom, lbuf, rbuf,
    x, f, fd, g, c_own, c_left, c_right, halo_f, halo_x, keep, acc, part_mom,
    load_sem, send_sem, recv_sem, msend_sem, mrecv_sem,
):
    vectors, _, _, rows, cols = vec.shape
    tall = x.shape[3]
    tiles = cols // LANES
    last = rows - EDGE
    gx = lax.axis_index("gx")
    gy = lax.axis_index("gy")

    def peer(dx, dy):
        return (lax.rem(gx + dx + gxn, gxn), lax.rem(gy + dy + gyn, gyn))

    loads = [
        pltpu.make_async_copy(vec, x.at[:, :, :, 0:rows, :], load_sem.at[0]),
        pltpu.make_async_copy(bonds, f.at[0:3, 0:rows, :], load_sem.at[1]),
        pltpu.make_async_copy(onsite, f.at[3:5, 0:rows, :], load_sem.at[2]),
    ]
    for copy in loads:
        copy.start()
    barrier = pltpu.get_barrier_semaphore()
    near = [(dx % gxn, dy % gyn) for dx in (-1, 0, 1) for dy in (-1, 0, 1)]
    near += [(0, dy) for dy in range(gyn)]
    near = sorted(set(near) - {(0, 0)})
    for dx, dy in near:
        pl.semaphore_signal(barrier, inc=1, device_id=peer(dx, dy), device_id_type=MESH)

    sends = []

    def send(src, dst, dx, dy):
        n = len(sends)
        copy = pltpu.make_async_remote_copy(
            src_ref=src, dst_ref=dst, send_sem=send_sem.at[n], recv_sem=recv_sem.at[n],
            device_id=peer(dx, dy), device_id_type=MESH,
        )
        copy.start()
        sends.append(copy)

    for copy in loads:
        copy.wait()

    acc[...] = jnp.zeros_like(acc)
    pl.semaphore_wait(barrier, len(near))

    core = slice(0, rows)
    send(x.at[:, :, 0, 0:2, :], x.at[:, :, 0, rows : rows + 2, :], -1, 0)
    send(x.at[:, :, 1, rows - 2 : rows, :], x.at[:, :, 1, tall - 2 : tall, :], 1, 0)
    send(x.at[:, :, 1, 0:1, :], x.at[:, :, 1, rows : rows + 1, :], -1, 0)
    send(x.at[:, :, 0, rows - 1 : rows, :], x.at[:, :, 0, tall - 1 : tall, :], 1, 0)
    send(f.at[:, 0:2, :], f.at[:, rows : rows + 2, :], -1, 0)
    send(f.at[:, rows - 2 : rows, :], f.at[:, tall - 2 : tall, :], 1, 0)

    lane = lax.broadcasted_iota(jnp.int32, (rows, LANES), 1)
    spot = lax.rem(lane, HALF)

    def packed(items):
        total = jnp.zeros((rows, LANES), jnp.float32)
        for k, (first, final) in enumerate(items):
            both = jnp.where(lane < HALF, first, final)
            moved = pltpu.roll(both, GROUP * k + EDGE, 1)
            total = jnp.where(spot // GROUP == k, moved, total) if k else moved
        total = jnp.where(lane < HALF, total, pltpu.roll(total, HALF, 1))
        return total

    def edges(ref, *index):
        return ref[(*index, slice(0, rows), slice(0, LANES))], ref[
            (*index, slice(0, rows), slice(cols - LANES, cols))
        ]

    for sub in range(2):
        c_own[sub, 0:rows] = packed(
            [edges(x, v, p, sub) for v in range(vectors) for p in range(2)]
        )
    c_own[2, 0:rows] = packed([edges(f, k) for k in range(5)])

    send(c_own.at[:, core, :], c_right.at[:, core, :], 0, -1)
    send(c_own.at[:, core, :], c_left.at[:, core, :], 0, 1)
    top, bottom = c_own.at[:, 0:EDGE, :], c_own.at[:, last:rows, :]
    past, ahead = slice(rows, rows + EDGE), slice(tall - EDGE, tall)
    send(top, c_own.at[:, past, :], -1, 0)
    send(top, c_right.at[:, past, :], -1, -1)
    send(top, c_left.at[:, past, :], -1, 1)
    send(bottom, c_own.at[:, ahead, :], 1, 0)
    send(bottom, c_right.at[:, ahead, :], 1, -1)
    send(bottom, c_left.at[:, ahead, :], 1, 1)

    def scaled(i, t, item):
        g[0, i, :, tile(t)] = item * (1.0 / SCALE)
        g[1, i, :, tile(t)] = item * (2.0 / SCALE)
        if i < 5:
            g[2, i, :, tile(t)] = item * ((-1.0 if i else 2.0) / (SCALE * SCALE))

    def tile(t):
        return slice(t * LANES, (t + 1) * LANES)

    for copy in sends[4:6]:
        copy.wait_recv()
    for t in range(tiles):
        fd[0, :, tile(t)] = pltpu.roll(f[1, :, tile(t)], tall - 1, 0)
        for i, item in ((0, f[0, :, tile(t)]), (1, f[1, :, tile(t)]), (2, f[2, :, tile(t)]),
                        (3, fd[0, :, tile(t)]), (5, f[3, :, tile(t)]), (6, f[4, :, tile(t)])):
            scaled(i, t, item)
    for copy in sends[:4] + sends[6:]:
        copy.wait_recv()

    tlane = lax.broadcasted_iota(jnp.int32, (tall, LANES), 1)
    tspot = lax.rem(tlane, GROUP)
    from_left = (tlane < HALF) & (tspot < EDGE)
    from_right = (tlane >= HALF) & (tspot >= EDGE)

    def joined(k):
        return jnp.where(
            from_left, c_left[k], jnp.where(from_right, c_right[k], c_own[k])
        )

    def up(t):
        return pltpu.roll(t, 1, 0)

    def down(t):
        return pltpu.roll(t, t.shape[0] - 1, 0)

    field_tile = joined(2)
    tgroup = lax.rem(tlane, HALF)
    for k in range(5):
        t = pltpu.roll(field_tile, LANES - GROUP * k, 1) if k else field_tile
        t = jnp.where(tgroup < GROUP, t, 0.0)
        step = GROUP
        while step < HALF:
            t = t + pltpu.roll(t, step, 1)
            step *= 2
        halo_f[k] = t
    halo_f[5] = down(halo_f[1])
    halo_f[6] = pltpu.roll(halo_f[2], LANES - 1, 1)

    lane_last = tlane == LANES - 1
    lane_first = tlane == 0

    def tile(t):
        return slice(t * LANES, (t + 1) * LANES)

    after = pltpu.roll(halo_f[2], LANES - 1 - (HALF + EDGE), 1)
    for t in reversed(range(tiles)):
        turned = pltpu.roll(f[2, :, tile(t)], LANES - 1, 1)
        fd[1, :, tile(t)] = jnp.where(lane_last, after, turned)
        after = turned

    sixth = 1.0 / SCALE
    half_square = 0.5 * SCALE * SCALE
    for t in range(tiles):
        scaled(4, t, fd[1, :, tile(t)])

    def h_fields(width=tall):
        return tuple(halo_f[k] for k in (0, 1, 2, 5, 6))

    h_on = (halo_f[3], halo_f[4])

    def h_terms(a, b):
        return bond_terms(
            a, b, h_fields(), lambda t: pltpu.roll(t, 1, 1),
            lambda t: pltpu.roll(t, LANES - 1, 1), up, down,
        )

    def energy(a, b, terms, on, factor):
        a0, a12, b0, b12 = terms
        return (on[0] * a + (a0 + a12)) * factor, (on[1] * b + (b0 + b12)) * factor

    def speed(terms):
        a0, a12, b0, b12 = terms
        return a0 - 0.5 * a12, 0.5 * b12 - b0

    q0 = (joined(0), joined(1))
    t0 = h_terms(*q0)
    q1 = energy(*q0, t0, h_on, 1.0)
    m0 = speed(t0)
    h1 = energy(*q1, h_terms(*q1), h_on, 1.0)
    q2 = (h1[0] - half_square * q0[0], h1[1] - half_square * q0[1])
    m1 = energy(*m0, h_terms(*m0), h_on, sixth)
    for k, pair in enumerate((q0, q1, q2, m0, m1)):
        halo_x[k, 0], halo_x[k, 1] = pair

    short = slice(0, rows)

    def one_vector(v, carry):
        for part in range(2):
            turn_b = lax.rem(2 * LANES - (GROUP * (2 * v + part) + 1), LANES)
            turn_a = lax.rem(3 * LANES - 1 - (HALF + GROUP * (2 * v + part) + EDGE), LANES)

            def terms(pair, k, cut, w=None):
                a, b = pair
                rim_b = pltpu.roll(halo_x[k, 1], turn_b, 1)
                rim_a = pltpu.roll(halo_x[k, 0], turn_a, 1)
                keep_rows = (lambda t: t[0:rows]) if cut else (lambda t: t)
                first, final = keep_rows(lane_first), keep_rows(lane_last)
                size = short if cut else slice(0, tall)
                b_turn = [pltpu.roll(keep_rows(t), 1, 1) for t in b]
                a_turn = [pltpu.roll(keep_rows(t), LANES - 1, 1) for t in a]
                found = []
                for t in range(tiles):
                    prev = keep_rows(rim_b) if t == 0 else b_turn[t - 1]
                    nxt = keep_rows(rim_a) if t == tiles - 1 else a_turn[t + 1]
                    left = jnp.where(first, prev, b_turn[t])
                    right = jnp.where(final, nxt, a_turn[t])
                    if w is None:
                        f0, f1, f2 = (f[i, size, tile(t)] for i in range(3))
                        d1, d2 = fd[0, size, tile(t)], fd[1, size, tile(t)]
                    else:
                        f0, f1, f2, d1, d2 = (g[w, i, size, tile(t)] for i in range(5))
                    a0 = f0 * keep_rows(b[t])
                    a12 = f1 * keep_rows(up(b[t])) + f2 * left
                    b0 = f0 * keep_rows(a[t])
                    b12 = d1 * keep_rows(down(a[t])) + d2 * right
                    found.append((a0, a12, b0, b12))
                return found

            def stepped(pair, found, cut, w=None, minus=None, times=None):
                a_new, b_new = [], []
                size = short if cut else slice(0, tall)
                for t in range(tiles):
                    if w is None:
                        on = (f[3, size, tile(t)], f[4, size, tile(t)])
                    else:
                        on = (g[w, 5, size, tile(t)], g[w, 6, size, tile(t)])
                    a0, a12, b0, b12 = found[t]
                    a = on[0] * pair[0][t][size] + (a0 + a12)
                    b = on[1] * pair[1][t][size] + (b0 + b12)
                    if minus is not None:
                        less = [minus[i][t][size] for i in range(2)]
                        if times is not None:
                            less = [item * times for item in less]
                        a, b = a - less[0], b - less[1]
                    a_new.append(a)
                    b_new.append(b)
                return a_new, b_new

            def moved(found):
                both = [speed(item) for item in found]
                return [item[0] for item in both], [item[1] for item in both]

            def store(slot, pair):
                for sub in range(2):
                    for t in range(tiles):
                        keep[slot, part, sub, :, tile(t)] = pair[sub][t][0:rows]

            q0 = tuple([x[v, part, sub, :, tile(t)] for t in range(tiles)] for sub in range(2))
            t0 = terms(q0, 0, False)
            m0 = moved(t0)
            store(0, m0)
            q1 = stepped(q0, t0, False)
            t1 = terms(q1, 1, False)
            store(3, moved(t1))
            q2 = stepped(q1, t1, False, None, q0, half_square)
            n2 = [[], []]
            for a0, a12, b0, b12 in terms(q2, 2, True, 2):
                n2[0].append(a0 + a12)
                n2[1].append(-(b0 + b12))
            store(4, n2)
            m1 = stepped(m0, terms(m0, 3, False, 0), False, 0)
            store(1, m1)
            m2 = stepped(m1, terms(m1, 4, True, 1), True, 1, m0)
            store(2, m2)
            for sub in range(2):
                for t in range(tiles):
                    for buf, pair in ((lbuf, m2), (rbuf, n2)):
                        value = pair[sub][t]
                        value = -value if part == 0 else value
                        buf[v, 1 - part, sub, :, tile(t)] = value.astype(jnp.bfloat16)

        for r in range(0, rows, 8):
            band = slice(r, r + 8)
            sums = [[[acc[p, n, m, band, :] for m in range(MOMENTS)] for n in range(MOMENTS)] for p in range(2)]
            for sub in range(2):
                for t in range(tiles):
                    at = [[keep[s, p, sub, band, tile(t)] for p in range(2)] for s in range(5)]
                    for n in range(MOMENTS):
                        for m in range(MOMENTS):
                            left = at[n]
                            right = at[0] if m == 0 else at[2 + m]
                            sums[0][n][m] = sums[0][n][m] + (left[0] * right[0] + left[1] * right[1])
                            sums[1][n][m] = sums[1][n][m] + (left[0] * right[1] - left[1] * right[0])
            for p in range(2):
                for n in range(MOMENTS):
                    for m in range(MOMENTS):
                        acc[p, n, m, band, :] = sums[p][n][m]
        return carry

    lax.fori_loop(0, vectors, one_vector, 0)

    for p in range(2):
        for n in range(MOMENTS):
            acc[p, n, 1] = acc[p, n, 1] * sixth
    count = 2 * MOMENTS * MOMENTS * rows
    part_mom[0] = lax.dot_general(
        jnp.ones((8, LANES), jnp.float32), acc[...].reshape(count, LANES),
        (((1,), (1,)), ((), ())), precision=lax.Precision.HIGHEST,
        preferred_element_type=jnp.float32,
    )
    swaps = []
    for d in range(1, gyn):
        copy = pltpu.make_async_remote_copy(
            src_ref=part_mom.at[0, 0:1], dst_ref=part_mom.at[d, 0:1],
            send_sem=msend_sem.at[d - 1], recv_sem=mrecv_sem.at[d - 1],
            device_id=peer(0, d), device_id_type=MESH,
        )
        copy.start()
        swaps.append(copy)
    for copy in swaps:
        copy.wait_recv()
    total = part_mom[0]
    for d in range(1, gyn):
        total = total + part_mom[d]
    out_mom[...] = total / float(vectors * cols * gyn)
    for copy in sends + swaps:
        copy.wait_send()


def writer(total, lbuf, rbuf, out_mom, out_left, out_right, mom, out_sem):
    outs = [
        pltpu.make_async_copy(lbuf, out_left, out_sem.at[0]),
        pltpu.make_async_copy(rbuf, out_right, out_sem.at[1]),
    ]
    for copy in outs:
        copy.start()
    rows = mom.shape[3]
    for p in range(2):
        for n in range(MOMENTS):
            for m in range(MOMENTS):
                k = (p * MOMENTS + n) * MOMENTS + m
                mom[n, m, p : p + 1, :] = total[0:1, k * rows : (k + 1) * rows]
    outs.append(pltpu.make_async_copy(mom, out_mom, out_sem.at[2]))
    outs[2].start()
    for copy in outs:
        copy.wait()


def solution(mesh):
    gxn, gyn = mesh.shape["gx"], mesh.shape["gy"]

    def per_device(vectors, bonds, onsite):
        count, _, _, rows, cols = vectors.shape
        tall = rows + 8
        f32 = jnp.float32
        in_hbm = pl.BlockSpec(memory_space=pltpu.HBM)
        last = jax.ShapeDtypeStruct(vectors.shape, jnp.bfloat16)
        sends = 16
        in_vmem = pl.BlockSpec(memory_space=pltpu.VMEM)
        sums = (8, 2 * MOMENTS * MOMENTS * rows)
        made = pl.pallas_call(
            functools.partial(kernel, gxn, gyn),
            out_shape=(
                pltpu.VMEM(sums, f32),
                pltpu.VMEM(vectors.shape, jnp.bfloat16),
                pltpu.VMEM(vectors.shape, jnp.bfloat16),
            ),
            in_specs=[in_hbm] * 3,
            out_specs=(in_vmem,) * 3,
            scratch_shapes=[
                pltpu.VMEM((count, 2, 2, tall, cols), f32),
                pltpu.VMEM((5, tall, cols), f32),
                pltpu.VMEM((2, tall, cols), f32),
                pltpu.VMEM((3, 7, tall, cols), f32),
                pltpu.VMEM((3, tall, LANES), f32),
                pltpu.VMEM((3, tall, LANES), f32),
                pltpu.VMEM((3, tall, LANES), f32),
                pltpu.VMEM((7, tall, LANES), f32),
                pltpu.VMEM((5, 2, tall, LANES), f32),
                pltpu.VMEM((5, 2, 2, rows, cols), f32),
                pltpu.VMEM((2, MOMENTS, MOMENTS, rows, LANES), f32),
                pltpu.VMEM((gyn, *sums), f32),
                pltpu.SemaphoreType.DMA((3,)),
                pltpu.SemaphoreType.DMA((sends,)),
                pltpu.SemaphoreType.DMA((sends,)),
                pltpu.SemaphoreType.DMA((gyn - 1,)),
                pltpu.SemaphoreType.DMA((gyn - 1,)),
            ],
            compiler_params=pltpu.CompilerParams(
                collective_id=0, has_side_effects=True, vmem_limit_bytes=GRANT
            ),
        )(*(pltpu.with_memory_space_constraint(array, pltpu.HBM) for array in (vectors, bonds, onsite)))
        made = [pltpu.with_memory_space_constraint(array, pltpu.VMEM) for array in made]
        moments, left, right = pl.pallas_call(
            writer,
            out_shape=(
                jax.ShapeDtypeStruct((MOMENTS, MOMENTS, 2, rows), f32), last, last,
            ),
            in_specs=[in_vmem] * 3,
            out_specs=(in_hbm,) * 3,
            scratch_shapes=[
                pltpu.VMEM((MOMENTS, MOMENTS, 2, rows), f32),
                pltpu.SemaphoreType.DMA((3,)),
            ],
            compiler_params=pltpu.CompilerParams(vmem_limit_bytes=GRANT),
        )(*made)
        return jnp.transpose(moments, (2, 0, 1, 3)), left, right

    return jax.shard_map(
        per_device,
        mesh=mesh,
        in_specs=(P(None, None, None, "gx", "gy"), P(None, "gx", "gy"), P(None, "gx", "gy")),
        out_specs=(
            P(None, None, None, "gx"),
            P(None, None, None, "gx", "gy"),
            P(None, None, None, "gx", "gy"),
        ),
        check_vma=False,
    )
```

```python
import functools
import jax
import jax.numpy as jnp
from jax import lax
from jax.experimental import pallas as pl
from jax.experimental.pallas import tpu as pltpu
from jax.sharding import PartitionSpec as P

MOMENTS = 3
SCALE = 6.0
EDGE = 2
GROUP = 8
HALF = 64
LANES = 128
SUBS = 8
SLOTS = 5
UNROLL = 8
GRANT = 32 * 1024 * 1024
MESH = pl.DeviceIdType.MESH
SIXTH = 1.0 / SCALE
HALF_SQUARE = 0.5 * SCALE * SCALE
BENT_INNER = (2.0, -1.0, -1.0, -1.0, -1.0)
BENT_WINDOW = (2.0, -1.0, -1.0, 2.0, -1.0)


def tile(t):
    return slice(t * LANES, (t + 1) * LANES)


def up(t):
    return pltpu.roll(t, 1, 0)


def down(t):
    return pltpu.roll(t, t.shape[0] - 1, 0)


def speed(terms):
    a0, a12, b0, b12 = terms
    return a0 - 0.5 * a12, 0.5 * b12 - b0


def energy(pair, terms, on, factor=None):
    a0, a12, b0, b12 = terms
    a, b = on[0] * pair[0] + (a0 + a12), on[1] * pair[1] + (b0 + b12)
    return (a, b) if factor is None else (a * factor, b * factor)


def add_products(sums, left, right):
    for n in range(MOMENTS):
        for m in range(MOMENTS):
            (p, q), (r, s) = left[n], right[m]
            sums[0][n][m] = sums[0][n][m] + (p * r + q * s)
            sums[1][n][m] = sums[1][n][m] + (p * s - q * r)


def rights_of(at):
    return [at[0], at[3], at[4]]


def masked(mask, at):
    return [[jnp.where(mask, item, 0.0) for item in at[n]] for n in range(MOMENTS)]


def each_sum():
    return [(p, n, m) for p in range(2) for n in range(MOMENTS) for m in range(MOMENTS)]


def kernel(
    gxn, gyn, vec, bonds, onsite, out_mom, lbuf, rbuf,
    x, xe, f, fw, fo, hw, gb, gw, cc, c_own, c_left, c_right, hf, cv, bw, lk, keep, acc, acw, part_mom,
    load_sem, send_sem, recv_sem, msend_sem, mrecv_sem,
):
    vectors, _, _, rows, cols = vec.shape
    tall = c_own.shape[1]
    tiles = cols // LANES
    last = tiles - 1
    gx = lax.axis_index("gx")
    gy = lax.axis_index("gy")

    def peer(dx, dy):
        return (lax.rem(gx + dx + gxn, gxn), lax.rem(gy + dy + gyn, gyn))

    low, high = slice(0, EDGE), slice(SUBS - EDGE, SUBS)
    loads = [
        pltpu.make_async_copy(vec.at[:, :, :, 0:EDGE, :], xe.at[:, :, :, low, :], load_sem.at[0]),
        pltpu.make_async_copy(
            vec.at[:, :, :, rows - EDGE : rows, :], xe.at[:, :, :, high, :], load_sem.at[1]
        ),
        pltpu.make_async_copy(bonds, f.at[0:3], load_sem.at[2]),
        pltpu.make_async_copy(onsite, f.at[3:5], load_sem.at[3]),
        pltpu.make_async_copy(vec, x, load_sem.at[4]),
    ]
    for copy in loads:
        copy.start()

    barrier = pltpu.get_barrier_semaphore()
    near = [(0, dy) for dy in range(gyn)]
    near += [(dx % gxn, dy % gyn) for dx in (-1, 1) for dy in (-1, 0, 1)]
    near = [one for k, one in enumerate(near) if one != (0, 0) and one not in near[:k]]
    for dx, dy in near:
        pl.semaphore_signal(barrier, inc=1, device_id=peer(dx, dy), device_id_type=MESH)

    hw[:, :, 0, 1 : SUBS - EDGE, :] = jnp.zeros((vectors, 2, SUBS - EDGE - 1, cols), jnp.float32)
    hw[:, :, 1, EDGE : SUBS - 1, :] = jnp.zeros((vectors, 2, SUBS - EDGE - 1, cols), jnp.float32)
    acc[...] = jnp.zeros_like(acc)
    sends = []

    def send(src, dst, dx, dy):
        n = len(sends)
        copy = pltpu.make_async_remote_copy(
            src_ref=src, dst_ref=dst, send_sem=send_sem.at[n], recv_sem=recv_sem.at[n],
            device_id=peer(dx, dy), device_id_type=MESH,
        )
        copy.start()
        sends.append(copy)

    def packed(items):
        count = items[0][0].shape[0]
        lane = lax.broadcasted_iota(jnp.int32, (count, LANES), 1)
        spot = lax.rem(lane, HALF)
        total = None
        for k, (first, final) in enumerate(items):
            both = jnp.where(lane < HALF, first, final)
            moved = pltpu.roll(both, GROUP * k + GROUP // 2, 1)
            total = jnp.where(spot // GROUP == k, moved, total) if k else moved
        return jnp.where(lane < HALF, total, pltpu.roll(total, HALF, 1))

    def ends(ref, *index):
        return ref[(*index, slice(None), slice(0, LANES))], ref[
            (*index, slice(None), slice(cols - LANES, cols))
        ]

    sub8 = lax.broadcasted_iota(jnp.int32, (SUBS, LANES), 0)
    lane8 = lax.broadcasted_iota(jnp.int32, (SUBS, LANES), 1)

    def window_a(t):
        return jnp.where(
            sub8 < 4, pltpu.roll(t[0:SUBS], 1, 0), pltpu.roll(t[rows - SUBS : rows], SUBS - 2, 0)
        )

    def window_b(t):
        return jnp.where(
            sub8 < 4, pltpu.roll(t[0:SUBS], 2, 0), pltpu.roll(t[rows - SUBS : rows], SUBS - 1, 0)
        )

    for copy in loads[:4]:
        copy.wait()
    for p in range(2):
        for sub in range(2):
            cc[2 * p + sub] = packed([ends(xe, v, p, sub) for v in range(vectors)])

    def rim_rows(t):
        return jnp.where(sub8 < 4, t[0:SUBS], t[rows - SUBS : rows])

    cc[4] = packed([tuple(rim_rows(t) for t in ends(f, k)) for k in range(5)])
    pl.semaphore_wait(barrier, len(near))

    send(f.at[0:4, 0:2, :], fw.at[0:4, SUBS - 2 : SUBS, :], -1, 0)
    send(f.at[4:5, 0:1, :], fw.at[4:5, SUBS - 1 : SUBS, :], -1, 0)
    send(f.at[0:4, rows - 1 : rows, :], fw.at[0:4, 0:1, :], 1, 0)
    send(f.at[4:5, rows - 2 : rows, :], fw.at[4:5, 0:2, :], 1, 0)
    past, ahead = slice(rows, rows + EDGE), slice(tall - EDGE, tall)
    for dst, dy in ((c_right, -1), (c_left, 1), (c_own, 0)):
        send(cc.at[:, low, :], dst.at[:, past, :], -1, dy)
        send(cc.at[:, high, :], dst.at[:, ahead, :], 1, dy)
    send(xe.at[:, :, 0, 0:2, :], hw.at[:, :, 0, SUBS - 2 : SUBS, :], -1, 0)
    send(xe.at[:, :, 1, SUBS - 2 : SUBS, :], hw.at[:, :, 1, 0:2, :], 1, 0)
    send(xe.at[:, :, 1, 0:1, :], hw.at[:, :, 1, SUBS - 1 : SUBS, :], -1, 0)
    send(xe.at[:, :, 0, SUBS - 1 : SUBS, :], hw.at[:, :, 0, 0:1, :], 1, 0)

    core = slice(0, rows)
    loads[4].wait()
    for p in range(2):
        for sub in range(2):
            c_own[2 * p + sub, core] = packed([ends(x, v, p, sub) for v in range(vectors)])
    c_own[4, core] = packed([ends(f, k) for k in range(5)])
    send(c_own.at[:, core, :], c_right.at[:, core, :], 0, -1)
    send(c_own.at[:, core, :], c_left.at[:, core, :], 0, 1)

    def fill(g, bent, fields, t):
        for i, item in enumerate(fields):
            g[3, i, :, tile(t)] = item
            g[0, i, :, tile(t)] = item * SIXTH
            g[1, i, :, tile(t)] = item * (2.0 * SIXTH)
            if i < 5:
                g[2, i, :, tile(t)] = item * (bent[i] * SIXTH * SIXTH)

    def turned(items, shift):
        size = items[0].shape
        lane = lax.broadcasted_iota(jnp.int32, size, 1)
        rolled = [pltpu.roll(t, shift % LANES, 1) for t in items]
        if shift > 0:
            return [jnp.where(lane == 0, rolled[(t - 1) % tiles], rolled[t]) for t in range(tiles)]
        return [
            jnp.where(lane == LANES - 1, rolled[(t + 1) % tiles], rolled[t]) for t in range(tiles)
        ]

    sub_r = lax.broadcasted_iota(jnp.int32, (rows, LANES), 0)
    lane_r = lax.broadcasted_iota(jnp.int32, (rows, LANES), 1)
    shifted = turned([f[2, :, tile(t)] for t in range(tiles)], -1)
    for t in range(tiles):
        inner = jnp.where(sub_r == 0, 0.0, f[1, :, tile(t)])
        fill(
            gb,
            BENT_INNER,
            (f[0, :, tile(t)], inner, f[2, :, tile(t)], down(inner), shifted[t],
             f[3, :, tile(t)], f[4, :, tile(t)]),
            t,
        )
        for k in range(4):
            fo[k, :, tile(t)] = window_a(f[k, :, tile(t)])
        fo[4, :, tile(t)] = window_b(f[4, :, tile(t)])

    def inner_terms(a, b, w):
        left, right = turned(b, 1), turned(a, -1)
        found = []
        for t in range(tiles):
            f0, f1, f2, d1, d2 = (gb[w, i, :, tile(t)] for i in range(5))
            found.append((f0 * b[t], f1 * up(b[t]) + f2 * left[t], f0 * a[t], d1 * down(a[t]) + d2 * right[t]))
        return found

    def window_terms(a, b, w, leak=None):
        b_up, a_down = [down(t) for t in b], [up(t) for t in a]
        left, right = turned(b_up, 1), turned(a_down, -1)
        found = []
        for t in range(tiles):
            f0, f1, f2, d0, d2 = (gw[w, i, :, tile(t)] for i in range(5))
            over_a = a[t] if leak is None else a[t] + leak[0][t]
            over_b = b[t] if leak is None else b[t] + leak[1][t]
            found.append((f0 * b_up[t], f1 * over_b + f2 * left[t], d0 * a_down[t], f1 * over_a + d2 * right[t]))
        return found

    def both(items):
        return [item[0] for item in items], [item[1] for item in items]

    def at_tile(pair, t):
        return pair[0][t], pair[1][t]

    def chains(q0, terms, g, leaks):
        def on(w, t):
            return g[w, 5, :, tile(t)], g[w, 6, :, tile(t)]

        def less(pair, other, times=None):
            return both(
                [
                    tuple(
                        one - (two if times is None else two * times)
                        for one, two in zip(at_tile(pair, t), at_tile(other, t))
                    )
                    for t in range(tiles)
                ]
            )

        def stepped(pair, found, w):
            return both([energy(at_tile(pair, t), found[t], on(w, t)) for t in range(tiles)])

        t0 = terms(*q0, 3, *leaks[0:1])
        m0 = both([speed(item) for item in t0])
        q1 = stepped(q0, t0, 3)
        t1 = terms(*q1, 3, *leaks[1:2])
        n1 = both([speed(item) for item in t1])
        q2 = less(stepped(q1, t1, 3), q0, HALF_SQUARE)
        n2 = both([(a0 + a12, -(b0 + b12)) for a0, a12, b0, b12 in terms(*q2, 2)])
        m1 = stepped(m0, terms(*m0, 0, *leaks[2:3]), 0)
        m2 = less(stepped(m1, terms(*m1, 1), 1), m0)
        return q1, (m0, m1, m2, n1, n2)

    def block_edge(t, size):
        lane = lax.broadcasted_iota(jnp.int32, size, 1)
        keep_lanes = None
        if t == 0:
            keep_lanes = lane >= EDGE
        if t == last:
            end = lane < LANES - EDGE
            keep_lanes = end if keep_lanes is None else keep_lanes & end
        return keep_lanes

    def lefts_inside(at, t):
        mask = block_edge(t, (SUBS, LANES))
        return at[:MOMENTS] if mask is None else masked(mask, at)

    def one_vector(v, carry):
        for p in range(2):
            q0 = tuple([x[v, p, sub, :, tile(t)] for t in range(tiles)] for sub in range(2))
            q1, slots = chains(q0, inner_terms, gb, ())
            for s, pair in enumerate(slots):
                for t in range(tiles):
                    for sub in range(2):
                        keep[s, p, sub, :, tile(t)] = pair[sub][t]
                    bw[v, p, s, 0, :, tile(t)] = window_a(pair[0][t])
                    bw[v, p, s, 1, :, tile(t)] = window_b(pair[1][t])
            for s, pair in enumerate((q0, q1, slots[0])):
                for t in range(tiles):
                    lk[v, p, s, 0, :, tile(t)] = jnp.where(sub8 == 1, window_a(pair[0][t]), 0.0)
                    lk[v, p, s, 1, :, tile(t)] = jnp.where(sub8 == 6, window_b(pair[1][t]), 0.0)
            for buf, pair in ((lbuf, slots[2]), (rbuf, slots[4])):
                for sub in range(2):
                    for t in range(tiles):
                        value = -pair[sub][t] if p == 0 else pair[sub][t]
                        buf[v, 1 - p, sub, :, tile(t)] = value.astype(jnp.bfloat16)

        for r in range(0, rows, SUBS):
            band = slice(r, r + SUBS)
            sums = [[[acc[p, n, m, band, :] for m in range(MOMENTS)] for n in range(MOMENTS)] for p in range(2)]
            for sub in range(2):
                for t in range(tiles):
                    at = [[keep[s, p, sub, band, tile(t)] for p in range(2)] for s in range(SLOTS)]
                    add_products(sums, lefts_inside(at, t), rights_of(at))
            for p, n, m in each_sum():
                acc[p, n, m, band, :] = sums[p][n][m]
        return carry

    lax.fori_loop(0, vectors, one_vector, 0)

    for copy in sends[:4]:
        copy.wait_recv()

    taken_a = (sub8 < 1) | (sub8 >= SUBS - 2)
    taken_b = (sub8 < 2) | (sub8 >= SUBS - 1)
    cut = (sub8 == 3) | (sub8 == SUBS - 1)
    windows = [
        [jnp.where(taken_b if k == 4 else taken_a, fw[k, :, tile(t)], fo[k, :, tile(t)]) for t in range(tiles)]
        for k in range(5)
    ]
    for k in (0, 2):
        windows[k] = [jnp.where(cut, 0.0, t) for t in windows[k]]
    far = turned([up(t) for t in windows[2]], -1)
    for t in range(tiles):
        fill(
            gw,
            BENT_WINDOW,
            (windows[0][t], windows[1][t], windows[2][t], up(windows[0][t]), far[t], windows[3][t], windows[4][t]),
            t,
        )

    for copy in sends[4:10] + sends[14:16]:
        copy.wait_recv()

    tlane = lax.broadcasted_iota(jnp.int32, (tall, LANES), 1)
    tspot = lax.rem(tlane, GROUP)
    from_left = (tlane < HALF) & (tspot < GROUP // 2)
    from_right = (tlane >= HALF) & (tspot >= GROUP // 2)

    def joined(k):
        return jnp.where(from_left, c_left[k], jnp.where(from_right, c_right[k], c_own[k]))

    field_tile = joined(4)
    place = (tlane // HALF) * HALF + tspot
    for k in range(5):
        hf[k] = jnp.take_along_axis(field_tile, place + GROUP * k, axis=1)
    hf[5] = down(hf[1])
    hf[6] = jnp.take_along_axis(field_tile, lax.rem(place + (2 * GROUP + 1), LANES), axis=1)
    h_on = (hf[3], hf[4])

    def rim_terms(a, b):
        f0, f1, f2, d1, d2 = hf[0], hf[1], hf[2], hf[5], hf[6]
        return (
            f0 * b, f1 * up(b) + f2 * pltpu.roll(b, 1, 1),
            f0 * a, d1 * down(a) + d2 * pltpu.roll(a, LANES - 1, 1),
        )

    for p in range(2):
        q0 = (joined(2 * p), joined(2 * p + 1))
        t0 = rim_terms(*q0)
        m0 = speed(t0)
        q1 = energy(q0, t0, h_on)
        t1 = rim_terms(*q1)
        n1 = speed(t1)
        h1 = energy(q1, t1, h_on)
        q2 = (h1[0] - HALF_SQUARE * q0[0], h1[1] - HALF_SQUARE * q0[1])
        n2 = tuple(item / HALF_SQUARE for item in speed(rim_terms(*q2)))
        m1 = energy(m0, rim_terms(*m0), h_on, SIXTH)
        h2 = energy(m1, rim_terms(*m1), h_on, 2.0 * SIXTH)
        m2 = (h2[0] - m0[0], h2[1] - m0[1])
        for s, pair in enumerate((m0, m1, m2, n1, n2)):
            for sub in range(2):
                cv[s, p, sub] = pair[sub][0:rows]

    spot8 = lax.rem(lane8, GROUP)
    rim_lanes = ((lane8 < HALF) & ((spot8 == 4) | (spot8 == 5))) | (
        (lane8 >= HALF) & ((spot8 == 2) | (spot8 == 3))
    )

    for copy in sends[10:14]:
        copy.wait_recv()

    def one_window(v):
        for p in range(2):
            q0 = tuple([hw[v, p, sub, :, tile(t)] for t in range(tiles)] for sub in range(2))
            leaks = [
                tuple([lk[v, p, s, sub, :, tile(t)] for t in range(tiles)] for sub in range(2))
                for s in range(3)
            ]
            _, slots = chains(q0, window_terms, gw, leaks)
            for s, pair in enumerate(slots):
                for sub in range(2):
                    for t in range(tiles):
                        bw[v, p, s, sub, :, tile(t)] = bw[v, p, s, sub, :, tile(t)] + pair[sub][t]

    def some_windows(i, carry):
        for j in range(UNROLL):
            one_window(i * UNROLL + j)
        return carry

    if UNROLL == vectors:
        some_windows(0, 0)
    else:
        lax.fori_loop(0, vectors // UNROLL, some_windows, 0)

    def none():
        zero = jnp.zeros((SUBS, LANES), jnp.float32)
        return [[[zero for _ in range(MOMENTS)] for _ in range(MOMENTS)] for _ in range(2)]

    for sub in range(2):
        sums = none()
        for v in range(vectors):
            for t in range(tiles):
                at = [[bw[v, p, s, sub, :, tile(t)] for p in range(2)] for s in range(SLOTS)]
                add_products(sums, lefts_inside(at, t), rights_of(at))
        for p, n, m in each_sum():
            acw[sub, p, n, m] = sums[p][n][m]

    for r in range(0, rows, SUBS):
        band = slice(r, r + SUBS)
        sums = none()
        for sub in range(2):
            at = [[cv[s, p, sub, band] for p in range(2)] for s in range(SLOTS)]
            add_products(sums, masked(rim_lanes, at), rights_of(at))
        for p, n, m in each_sum():
            value = acc[p, n, m, band, :]
            if r == 0 or r == rows - SUBS:
                over = acw[0, p, n, m] + pltpu.roll(acw[1, p, n, m], SUBS - 1, 0)
                if r == 0:
                    value = jnp.where(sub8 < EDGE, pltpu.roll(over, SUBS - 1, 0), value)
                if r == rows - SUBS:
                    value = jnp.where(sub8 >= SUBS - EDGE, pltpu.roll(over, 2, 0), value)
            value = value + sums[p][n][m]
            acc[p, n, m, band, :] = value * SIXTH if m == 1 else value

    count = 2 * MOMENTS * MOMENTS * rows
    rest = acc[...].reshape(count, LANES)
    ones = jnp.ones((SUBS, LANES), jnp.bfloat16)
    total = None
    for _ in range(3):
        piece = rest.astype(jnp.bfloat16)
        rest = rest - piece.astype(jnp.float32)
        part = lax.dot_general(
            ones, piece, (((1,), (1,)), ((), ())), preferred_element_type=jnp.float32
        )
        total = part if total is None else total + part
    part_mom[0] = total
    swaps = []
    for d in range(1, gyn):
        copy = pltpu.make_async_remote_copy(
            src_ref=part_mom.at[0, 0:1], dst_ref=part_mom.at[d, 0:1],
            send_sem=msend_sem.at[d - 1], recv_sem=mrecv_sem.at[d - 1],
            device_id=peer(0, d), device_id_type=MESH,
        )
        copy.start()
        swaps.append(copy)

    def patch(v, carry):
        turn_first = lax.rem(2 * LANES - GROUP // 2 - GROUP * v, LANES)
        turn_last = lax.rem(2 * LANES - GROUP // 2 + HALF - GROUP * v, LANES)
        for p in range(2):
            for sub in range(2):
                for s, buf in ((2, lbuf), (4, rbuf)):
                    side = cv[s, p, sub]
                    for t in range(tiles):
                        value = buf[v, 1 - p, sub, :, tile(t)].astype(jnp.float32)
                        over = bw[v, p, s, sub, :, tile(t)]
                        edge = -side if p == 0 else side
                        over = -over if p == 0 else over
                        top = jnp.where(sub8 < EDGE, pltpu.roll(over, SUBS - 1 - sub, 0), value[0:SUBS])
                        bottom = jnp.where(
                            sub8 >= SUBS - EDGE, pltpu.roll(over, 2 - sub, 0), value[rows - SUBS : rows]
                        )
                        value = jnp.concatenate([top, value[SUBS : rows - SUBS], bottom] if rows > 2 * SUBS else [top, bottom], 0)
                        if t == 0:
                            value = jnp.where(lane_r < EDGE, pltpu.roll(edge, turn_first, 1), value)
                        if t == last:
                            value = jnp.where(lane_r >= LANES - EDGE, pltpu.roll(edge, turn_last, 1), value)
                        buf[v, 1 - p, sub, :, tile(t)] = value.astype(jnp.bfloat16)
        return carry

    lax.fori_loop(0, vectors, patch, 0)

    for copy in swaps:
        copy.wait_recv()
    total = part_mom[0]
    for d in range(1, gyn):
        total = total + part_mom[d]
    out_mom[...] = total / float(vectors * cols * gyn)
    for copy in sends + swaps:
        copy.wait_send()


def writer(total, lbuf, rbuf, out_mom, out_left, out_right, mom, out_sem):
    outs = [
        pltpu.make_async_copy(lbuf, out_left, out_sem.at[0]),
        pltpu.make_async_copy(rbuf, out_right, out_sem.at[1]),
    ]
    for copy in outs:
        copy.start()
    rows = mom.shape[3]
    for p in range(2):
        for n in range(MOMENTS):
            for m in range(MOMENTS):
                k = (p * MOMENTS + n) * MOMENTS + m
                mom[n, m, p : p + 1, :] = total[0:1, k * rows : (k + 1) * rows]
    outs.append(pltpu.make_async_copy(mom, out_mom, out_sem.at[2]))
    outs[2].start()
    for copy in outs:
        copy.wait()


def solution(mesh):
    gxn, gyn = mesh.shape["gx"], mesh.shape["gy"]

    def per_device(vectors, bonds, onsite):
        count, _, _, rows, cols = vectors.shape
        tall = rows + 8
        f32 = jnp.float32
        in_hbm = pl.BlockSpec(memory_space=pltpu.HBM)
        last = jax.ShapeDtypeStruct(vectors.shape, jnp.bfloat16)
        sends = 16
        in_vmem = pl.BlockSpec(memory_space=pltpu.VMEM)
        sums = (8, 2 * MOMENTS * MOMENTS * rows)
        made = pl.pallas_call(
            functools.partial(kernel, gxn, gyn),
            out_shape=(
                pltpu.VMEM(sums, f32),
                pltpu.VMEM(vectors.shape, jnp.bfloat16),
                pltpu.VMEM(vectors.shape, jnp.bfloat16),
            ),
            in_specs=[in_hbm] * 3,
            out_specs=(in_vmem,) * 3,
            scratch_shapes=[
                pltpu.VMEM(vectors.shape, f32),
                pltpu.VMEM((count, 2, 2, SUBS, cols), f32),
                pltpu.VMEM((5, rows, cols), f32),
                pltpu.VMEM((5, SUBS, cols), f32),
                pltpu.VMEM((5, SUBS, cols), f32),
                pltpu.VMEM((count, 2, 2, SUBS, cols), f32),
                pltpu.VMEM((4, 7, rows, cols), f32),
                pltpu.VMEM((4, 7, SUBS, cols), f32),
                pltpu.VMEM((5, SUBS, LANES), f32),
                pltpu.VMEM((5, tall, LANES), f32),
                pltpu.VMEM((5, tall, LANES), f32),
                pltpu.VMEM((5, tall, LANES), f32),
                pltpu.VMEM((7, tall, LANES), f32),
                pltpu.VMEM((SLOTS, 2, 2, rows, LANES), f32),
                pltpu.VMEM((count, 2, SLOTS, 2, SUBS, cols), f32),
                pltpu.VMEM((count, 2, 3, 2, SUBS, cols), f32),
                pltpu.VMEM((SLOTS, 2, 2, rows, cols), f32),
                pltpu.VMEM((2, MOMENTS, MOMENTS, rows, LANES), f32),
                pltpu.VMEM((2, 2, MOMENTS, MOMENTS, SUBS, LANES), f32),
                pltpu.VMEM((gyn, *sums), f32),
                pltpu.SemaphoreType.DMA((5,)),
                pltpu.SemaphoreType.DMA((sends,)),
                pltpu.SemaphoreType.DMA((sends,)),
                pltpu.SemaphoreType.DMA((gyn - 1,)),
                pltpu.SemaphoreType.DMA((gyn - 1,)),
            ],
            compiler_params=pltpu.CompilerParams(
                collective_id=0, has_side_effects=True, vmem_limit_bytes=GRANT
            ),
        )(*(pltpu.with_memory_space_constraint(array, pltpu.HBM) for array in (vectors, bonds, onsite)))
        made = [pltpu.with_memory_space_constraint(array, pltpu.VMEM) for array in made]
        moments, left, right = pl.pallas_call(
            writer,
            out_shape=(
                jax.ShapeDtypeStruct((MOMENTS, MOMENTS, 2, rows), f32), last, last,
            ),
            in_specs=[in_vmem] * 3,
            out_specs=(in_hbm,) * 3,
            scratch_shapes=[
                pltpu.VMEM((MOMENTS, MOMENTS, 2, rows), f32),
                pltpu.SemaphoreType.DMA((3,)),
            ],
            compiler_params=pltpu.CompilerParams(vmem_limit_bytes=GRANT),
        )(*made)
        return jnp.transpose(moments, (2, 0, 1, 3)), left, right

    return jax.shard_map(
        per_device,
        mesh=mesh,
        in_specs=(P(None, None, None, "gx", "gy"), P(None, "gx", "gy"), P(None, "gx", "gy")),
        out_specs=(
            P(None, None, None, "gx"),
            P(None, None, None, "gx", "gy"),
            P(None, None, None, "gx", "gy"),
        ),
        check_vma=False,
    )
```

```python
import functools
import jax
import jax.numpy as jnp
from jax import lax
from jax.experimental import pallas as pl
from jax.experimental.pallas import tpu as pltpu
from jax.sharding import PartitionSpec as P

MOMENTS = 3
SCALE = 6.0
EDGE = 2
GROUP = 8
HALF = 64
LANES = 128
SUBS = 8
SLOTS = 5
GRANT = 32 * 1024 * 1024
MESH = pl.DeviceIdType.MESH
SIXTH = 1.0 / SCALE
HALF_SQUARE = 0.5 * SCALE * SCALE
BENT_INNER = (2.0, -1.0, -1.0, -1.0, -1.0)
BENT_WINDOW = (2.0, -1.0, -1.0, 2.0, -1.0)


def tile(t):
    return slice(t * LANES, (t + 1) * LANES)


def up(t):
    return pltpu.roll(t, 1, 0)


def down(t):
    return pltpu.roll(t, t.shape[0] - 1, 0)


def speed(terms):
    a0, a12, b0, b12 = terms
    return a0 - 0.5 * a12, 0.5 * b12 - b0


def energy(pair, terms, on, factor=None):
    a0, a12, b0, b12 = terms
    a, b = on[0] * pair[0] + (a0 + a12), on[1] * pair[1] + (b0 + b12)
    return (a, b) if factor is None else (a * factor, b * factor)


def add_products(sums, left, right):
    for n in range(MOMENTS):
        for m in range(MOMENTS):
            (p, q), (r, s) = left[n], right[m]
            sums[0][n][m] = sums[0][n][m] + (p * r + q * s)
            sums[1][n][m] = sums[1][n][m] + (p * s - q * r)


def rights_of(at):
    return [at[0], at[3], at[4]]


def masked(mask, at):
    return [[jnp.where(mask, item, 0.0) for item in at[n]] for n in range(MOMENTS)]


def each_sum():
    return [(p, n, m) for p in range(2) for n in range(MOMENTS) for m in range(MOMENTS)]


def kernel(
    gxn, gyn, vec, bonds, onsite, out_mom, lbuf, rbuf,
    x, xe, f, fw, fo, hw, gb, gw, cc, c_own, c_left, c_right, hf, cv, bw, lk, state, keep, acc, part_mom,
    load_sem, send_sem, recv_sem, msend_sem, mrecv_sem,
):
    vectors, _, _, rows, cols = vec.shape
    tall = c_own.shape[1]
    tiles = cols // LANES
    last = tiles - 1
    gx = lax.axis_index("gx")
    gy = lax.axis_index("gy")

    def peer(dx, dy):
        return (lax.rem(gx + dx + gxn, gxn), lax.rem(gy + dy + gyn, gyn))

    barrier = pltpu.get_barrier_semaphore()
    near = [(dx % gxn, dy % gyn) for dx in (-1, 1) for dy in (0, 1, -1)]
    near += [(0, dy) for dy in range(gyn)]
    near = [one for k, one in enumerate(near) if one != (0, 0) and one not in near[:k]]
    for dx, dy in near:
        pl.semaphore_signal(barrier, inc=1, device_id=peer(dx, dy), device_id_type=MESH)

    low, high = slice(0, EDGE), slice(SUBS - EDGE, SUBS)
    loads = [
        pltpu.make_async_copy(vec.at[:, :, :, 0:EDGE, :], xe.at[:, :, :, low, :], load_sem.at[0]),
        pltpu.make_async_copy(
            vec.at[:, :, :, rows - EDGE : rows, :], xe.at[:, :, :, high, :], load_sem.at[1]
        ),
        pltpu.make_async_copy(bonds, f.at[0:3], load_sem.at[2]),
        pltpu.make_async_copy(onsite, f.at[3:5], load_sem.at[3]),
        pltpu.make_async_copy(vec, x, load_sem.at[4]),
    ]
    for copy in loads:
        copy.start()

    hw[:, :, 0, 1 : SUBS - EDGE, :] = jnp.zeros((vectors, 2, SUBS - EDGE - 1, cols), jnp.float32)
    hw[:, :, 1, EDGE : SUBS - 1, :] = jnp.zeros((vectors, 2, SUBS - EDGE - 1, cols), jnp.float32)
    acc[...] = jnp.zeros_like(acc)
    sends = []

    def send(src, dst, dx, dy):
        n = len(sends)
        copy = pltpu.make_async_remote_copy(
            src_ref=src, dst_ref=dst, send_sem=send_sem.at[n], recv_sem=recv_sem.at[n],
            device_id=peer(dx, dy), device_id_type=MESH,
        )
        sends.append(copy)
        return copy

    def packed(items):
        count = items[0][0].shape[0]
        lane = lax.broadcasted_iota(jnp.int32, (count, LANES), 1)
        spot = lax.rem(lane, HALF)
        total = None
        for k, (first, final) in enumerate(items):
            both = jnp.where(lane < HALF, first, final)
            place = lax.rem(spot + (2 * LANES - GROUP * k - GROUP // 2), LANES)
            moved = jnp.take_along_axis(both, place, axis=1)
            total = jnp.where(spot // GROUP == k, moved, total) if k else moved
        return total

    def ends(ref, *index):
        return ref[(*index, slice(None), slice(0, LANES))], ref[
            (*index, slice(None), slice(cols - LANES, cols))
        ]

    sub8 = lax.broadcasted_iota(jnp.int32, (SUBS, LANES), 0)
    lane8 = lax.broadcasted_iota(jnp.int32, (SUBS, LANES), 1)

    def window_a(t):
        return jnp.where(
            sub8 < 4, pltpu.roll(t[0:SUBS], 1, 0), pltpu.roll(t[rows - SUBS : rows], SUBS - 2, 0)
        )

    def window_b(t):
        return jnp.where(
            sub8 < 4, pltpu.roll(t[0:SUBS], 2, 0), pltpu.roll(t[rows - SUBS : rows], SUBS - 1, 0)
        )

    for copy in loads[:4]:
        copy.wait()
    for p in range(2):
        for sub in range(2):
            cc[2 * p + sub] = packed([ends(xe, v, p, sub) for v in range(vectors)])

    def rim_rows(t):
        return jnp.where(sub8 < 4, t[0:SUBS], t[rows - SUBS : rows])

    cc[4] = packed([tuple(rim_rows(t) for t in ends(f, k)) for k in range(5)])
    lane_r = lax.broadcasted_iota(jnp.int32, (rows, LANES), 1)
    core = slice(0, rows)

    def pack_block():
        loads[4].wait()
        for p in range(2):
            for sub in range(2):
                c_own[2 * p + sub, core] = packed([ends(x, v, p, sub) for v in range(vectors)])
        c_own[4, core] = packed([ends(f, k) for k in range(5)])

    def fill(g, bent, fields, t):
        for i, item in enumerate(fields):
            g[3, i, :, tile(t)] = item
            g[0, i, :, tile(t)] = item * SIXTH
            g[1, i, :, tile(t)] = item * (2.0 * SIXTH)
            if i < 5:
                g[2, i, :, tile(t)] = item * (bent[i] * SIXTH * SIXTH)

    def turned(items, shift):
        size = items[0].shape
        lane = lax.broadcasted_iota(jnp.int32, size, 1)
        rolled = [pltpu.roll(t, shift % LANES, 1) for t in items]
        if shift > 0:
            return rolled[:1] + [jnp.where(lane == 0, rolled[t - 1], rolled[t]) for t in range(1, tiles)]
        return [
            jnp.where(lane == LANES - 1, rolled[t + 1], rolled[t]) for t in range(last)
        ] + rolled[last:]

    def inner_terms(a, b, w):
        left, right = turned(b, 1), turned(a, -1)
        found = []
        for t in range(tiles):
            f0, f1, f2, d1, d2 = (gb[w, i, :, tile(t)] for i in range(5))
            found.append((f0 * b[t], f1 * up(b[t]) + f2 * left[t], f0 * a[t], d1 * down(a[t]) + d2 * right[t]))
        return found

    def window_terms(a, b, w, leak=None):
        b_up, a_down = [down(t) for t in b], [up(t) for t in a]
        left, right = turned(b_up, 1), turned(a_down, -1)
        found = []
        for t in range(tiles):
            f0, f1, f2, d0, d2 = (gw[w, i, :, tile(t)] for i in range(5))
            over_a = a[t] if leak is None else a[t] + leak[0][t]
            over_b = b[t] if leak is None else b[t] + leak[1][t]
            found.append((f0 * b_up[t], f1 * over_b + f2 * left[t], d0 * a_down[t], f1 * over_a + d2 * right[t]))
        return found

    def both(items):
        return [item[0] for item in items], [item[1] for item in items]

    def at_tile(pair, t):
        return pair[0][t], pair[1][t]

    def chains(q0, terms, g, leaks):
        def on(w, t):
            return g[w, 5, :, tile(t)], g[w, 6, :, tile(t)]

        def less(pair, other, times=None):
            return both(
                [
                    tuple(
                        one - (two if times is None else two * times)
                        for one, two in zip(at_tile(pair, t), at_tile(other, t))
                    )
                    for t in range(tiles)
                ]
            )

        def stepped(pair, found, w):
            return both([energy(at_tile(pair, t), found[t], on(w, t)) for t in range(tiles)])

        t0 = terms(*q0, 3, *leaks[0:1])
        m0 = both([speed(item) for item in t0])
        q1 = stepped(q0, t0, 3)
        t1 = terms(*q1, 3, *leaks[1:2])
        n1 = both([speed(item) for item in t1])
        q2 = less(stepped(q1, t1, 3), q0, HALF_SQUARE)
        n2 = both([(a0 + a12, -(b0 + b12)) for a0, a12, b0, b12 in terms(*q2, 2)])
        m1 = stepped(m0, terms(*m0, 0, *leaks[2:3]), 0)
        m2 = less(stepped(m1, terms(*m1, 1), 1), m0)
        return q1, (m0, m1, m2, n1, n2)

    def inside_lanes(t):
        keep_lanes = None
        if t == 0:
            keep_lanes = lane8 >= EDGE
        if t == last:
            end = lane8 < LANES - EDGE
            keep_lanes = end if keep_lanes is None else keep_lanes & end
        return keep_lanes

    def inside(sub, r, t):
        keep_cells = inside_lanes(t)
        cuts = []
        if r == 0:
            cuts.append(sub8 >= EDGE - sub)
        if r == rows - SUBS:
            cuts.append(sub8 < SUBS - 1 - sub)
        for one in cuts:
            keep_cells = one if keep_cells is None else keep_cells & one
        return keep_cells

    def one_vector(v, carry):
        for p in range(2):
            q0 = tuple([x[v, p, sub, :, tile(t)] for t in range(tiles)] for sub in range(2))
            q1, slots = chains(q0, inner_terms, gb, ())
            for s, pair in enumerate(slots):
                for t in range(tiles):
                    for sub in range(2):
                        keep[s, p, sub, :, tile(t)] = pair[sub][t]
                    a, b = pair[0][t], pair[1][t]
                    ends_a, ends_b = (a[0:SUBS], a[rows - SUBS : rows]), (b[0:SUBS], b[rows - SUBS : rows])
                    over = jnp.where(sub8 == 3, pltpu.roll(ends_b[0], 3, 0), ends_b[1])
                    over = jnp.where(sub8 == 5, pltpu.roll(ends_a[1], SUBS - 2, 0), over)
                    bw[v, p, s, :, tile(t)] = jnp.where(
                        (sub8 == 1) | (sub8 == 2), pltpu.roll(ends_a[0], 1, 0), over
                    )
            for s, pair in enumerate((q0, q1, slots[0])):
                for t in range(tiles):
                    lk[v, p, s, 0, :, tile(t)] = jnp.where(sub8 == 1, window_a(pair[0][t]), 0.0)
                    lk[v, p, s, 1, :, tile(t)] = jnp.where(sub8 == 6, window_b(pair[1][t]), 0.0)
            for buf, pair in ((lbuf, slots[2]), (rbuf, slots[4])):
                for sub in range(2):
                    for t in range(tiles):
                        value = -pair[sub][t] if p == 0 else pair[sub][t]
                        buf[v, 1 - p, sub, :, tile(t)] = value.astype(jnp.bfloat16)

        for r in range(0, rows, SUBS):
            band = slice(r, r + SUBS)
            sums = [[[acc[p, n, m, band, :] for m in range(MOMENTS)] for n in range(MOMENTS)] for p in range(2)]
            for sub in range(2):
                for t in range(tiles):
                    at = [[keep[s, p, sub, band, tile(t)] for p in range(2)] for s in range(SLOTS)]
                    mask = inside(sub, r, t)
                    add_products(sums, at[:MOMENTS] if mask is None else masked(mask, at), rights_of(at))
            for p, n, m in each_sum():
                acc[p, n, m, band, :] = sums[p][n][m]
        return carry

    def own_block():
        sub_r = lax.broadcasted_iota(jnp.int32, (rows, LANES), 0)
        shifted = turned([f[2, :, tile(t)] for t in range(tiles)], -1)
        for t in range(tiles):
            inner = jnp.where(sub_r == 0, 0.0, f[1, :, tile(t)])
            fill(
                gb,
                BENT_INNER,
                (f[0, :, tile(t)], inner, f[2, :, tile(t)], down(inner), shifted[t],
                 f[3, :, tile(t)], f[4, :, tile(t)]),
                t,
            )
            for k in range(4):
                fo[k, :, tile(t)] = window_a(f[k, :, tile(t)])
            fo[4, :, tile(t)] = window_b(f[4, :, tile(t)])
        lax.fori_loop(0, vectors, one_vector, 0)

    early = gx == 0

    @pl.when(early)
    def _():
        pack_block()
        own_block()

    pl.semaphore_wait(barrier, len(near))

    past, ahead = slice(rows, rows + EDGE), slice(tall - EDGE, tall)
    sides = [
        send(c_own.at[:, core, :], c_right.at[:, core, :], 0, -1),
        send(c_own.at[:, core, :], c_left.at[:, core, :], 0, 1),
    ]
    rims = [
        send(f.at[0:4, rows - 1 : rows, :], fw.at[0:4, 0:1, :], 1, 0),
        send(f.at[4:5, rows - 2 : rows, :], fw.at[4:5, 0:2, :], 1, 0),
    ]
    for dst, dy in ((c_right, -1), (c_left, 1), (c_own, 0)):
        rims.append(send(cc.at[:, high, :], dst.at[:, ahead, :], 1, dy))
    rims += [
        send(xe.at[:, :, 1, SUBS - 2 : SUBS, :], hw.at[:, :, 1, 0:2, :], 1, 0),
        send(xe.at[:, :, 0, SUBS - 1 : SUBS, :], hw.at[:, :, 0, 0:1, :], 1, 0),
        send(f.at[0:4, 0:2, :], fw.at[0:4, SUBS - 2 : SUBS, :], -1, 0),
        send(f.at[4:5, 0:1, :], fw.at[4:5, SUBS - 1 : SUBS, :], -1, 0),
    ]
    for dst, dy in ((c_right, -1), (c_left, 1), (c_own, 0)):
        rims.append(send(cc.at[:, low, :], dst.at[:, past, :], -1, dy))
    rims += [
        send(xe.at[:, :, 0, 0:2, :], hw.at[:, :, 0, SUBS - 2 : SUBS, :], -1, 0),
        send(xe.at[:, :, 1, 0:1, :], hw.at[:, :, 1, SUBS - 1 : SUBS, :], -1, 0),
    ]

    @pl.when(early)
    def _():
        for copy in sides:
            copy.start()

    for copy in rims:
        copy.start()

    @pl.when(jnp.logical_not(early))
    def _():
        pack_block()
        for copy in sides:
            copy.start()
        own_block()

    for copy in sends:
        copy.wait_recv()

    taken_a = (sub8 < 1) | (sub8 >= SUBS - 2)
    taken_b = (sub8 < 2) | (sub8 >= SUBS - 1)
    cut = (sub8 == 3) | (sub8 == SUBS - 1)
    windows = [
        [jnp.where(taken_b if k == 4 else taken_a, fw[k, :, tile(t)], fo[k, :, tile(t)]) for t in range(tiles)]
        for k in range(5)
    ]
    for k in (0, 2):
        windows[k] = [jnp.where(cut, 0.0, t) for t in windows[k]]
    far = turned([up(t) for t in windows[2]], -1)
    for t in range(tiles):
        fill(
            gw,
            BENT_WINDOW,
            (windows[0][t], windows[1][t], windows[2][t], up(windows[0][t]), far[t], windows[3][t], windows[4][t]),
            t,
        )


    tlane = lax.broadcasted_iota(jnp.int32, (tall, LANES), 1)
    tspot = lax.rem(tlane, GROUP)
    from_left = (tlane < HALF) & (tspot < GROUP // 2)
    from_right = (tlane >= HALF) & (tspot >= GROUP // 2)

    def joined(k):
        return jnp.where(from_left, c_left[k], jnp.where(from_right, c_right[k], c_own[k]))

    field_tile = joined(4)
    place = (tlane // HALF) * HALF + tspot
    for k in range(5):
        hf[k] = jnp.take_along_axis(field_tile, place + GROUP * k, axis=1)
    hf[5] = down(hf[1])
    hf[6] = jnp.take_along_axis(field_tile, lax.rem(place + (2 * GROUP + 1), LANES), axis=1)
    h_on = (hf[3], hf[4])

    def rim_terms(a, b):
        f0, f1, f2, d1, d2 = hf[0], hf[1], hf[2], hf[5], hf[6]
        return (
            f0 * b, f1 * up(b) + f2 * pltpu.roll(b, 1, 1),
            f0 * a, d1 * down(a) + d2 * pltpu.roll(a, LANES - 1, 1),
        )

    for p in range(2):
        q0 = (joined(2 * p), joined(2 * p + 1))
        t0 = rim_terms(*q0)
        m0 = speed(t0)
        q1 = energy(q0, t0, h_on)
        t1 = rim_terms(*q1)
        n1 = speed(t1)
        h1 = energy(q1, t1, h_on)
        q2 = (h1[0] - HALF_SQUARE * q0[0], h1[1] - HALF_SQUARE * q0[1])
        n2 = tuple(item / HALF_SQUARE for item in speed(rim_terms(*q2)))
        m1 = energy(m0, rim_terms(*m0), h_on, SIXTH)
        h2 = energy(m1, rim_terms(*m1), h_on, 2.0 * SIXTH)
        m2 = (h2[0] - m0[0], h2[1] - m0[1])
        for s, pair in enumerate((m0, m1, m2, n1, n2)):
            for sub in range(2):
                cv[s, p, sub] = pair[sub][0:rows]

    spot8 = lax.rem(lane8, GROUP)
    rim_lanes = ((lane8 < HALF) & ((spot8 == 4) | (spot8 == 5))) | (
        (lane8 >= HALF) & ((spot8 == 2) | (spot8 == 3))
    )


    def none():
        zero = jnp.zeros((SUBS, LANES), jnp.float32)
        return [[[zero for _ in range(MOMENTS)] for _ in range(MOMENTS)] for _ in range(2)]

    from_a = (sub8 == 1) | (sub8 == 2) | (sub8 == 5)
    planes = [(v, p) for v in range(vectors) for p in range(2)]

    def pair_of(ref, *index):
        return tuple([ref[(*index, sub, slice(None), tile(t))] for t in range(tiles)] for sub in range(2))

    def on_window(pair, found, w):
        return both(
            [
                energy(at_tile(pair, t), found[t], (gw[w, 5, :, tile(t)], gw[w, 6, :, tile(t)]))
                for t in range(tiles)
            ]
        )

    def put(k, v, p, pair):
        for sub in range(2):
            for t in range(tiles):
                state[k, v, p, sub, :, tile(t)] = pair[sub][t]

    def add(v, p, s, pair):
        for t in range(tiles):
            change = jnp.where(from_a, pair[0][t], up(pair[1][t]))
            bw[v, p, s, :, tile(t)] = bw[v, p, s, :, tile(t)] + change

    def minus(pair, other, times=None):
        return tuple(
            [one - (two if times is None else two * times) for one, two in zip(pair[sub], other[sub])]
            for sub in range(2)
        )

    for v, p in planes:
        pair = pair_of(hw, v, p)
        found = window_terms(*pair, 3, pair_of(lk, v, p, 0))
        m0 = both([speed(item) for item in found])
        put(0, v, p, on_window(pair, found, 3))
        put(1, v, p, m0)
        add(v, p, 0, m0)
    for v, p in planes:
        pair = pair_of(state, 0, v, p)
        found = window_terms(*pair, 3, pair_of(lk, v, p, 1))
        add(v, p, 3, both([speed(item) for item in found]))
        put(2, v, p, minus(on_window(pair, found, 3), pair_of(hw, v, p), HALF_SQUARE))
    for v, p in planes:
        pair = pair_of(state, 1, v, p)
        m1 = on_window(pair, window_terms(*pair, 0, pair_of(lk, v, p, 2)), 0)
        put(3, v, p, m1)
        add(v, p, 1, m1)
    for v, p in planes:
        found = window_terms(*pair_of(state, 2, v, p), 2)
        add(v, p, 4, both([(a0 + a12, -(b0 + b12)) for a0, a12, b0, b12 in found]))
    for v, p in planes:
        pair = pair_of(state, 3, v, p)
        add(v, p, 2, minus(on_window(pair, window_terms(*pair, 1), 1), pair_of(state, 1, v, p)))

    found = none()
    for t in range(tiles):
        sums = none()
        for v in range(vectors):
            at = [[bw[v, p, s, :, tile(t)] for p in range(2)] for s in range(SLOTS)]
            add_products(sums, at[:MOMENTS], rights_of(at))
        mask = inside_lanes(t)
        for p, n, m in each_sum():
            value = sums[p][n][m] if mask is None else jnp.where(mask, sums[p][n][m], 0.0)
            found[p][n][m] = value if t == 0 else found[p][n][m] + value
    for r in range(0, rows, SUBS):
        band = slice(r, r + SUBS)
        sums = none()
        for sub in range(2):
            at = [[cv[s, p, sub, band] for p in range(2)] for s in range(SLOTS)]
            add_products(sums, masked(rim_lanes, at), rights_of(at))
        for p, n, m in each_sum():
            value = acc[p, n, m, band, :] + sums[p][n][m]
            acc[p, n, m, band, :] = value * SIXTH if m == 1 else value

    count = 2 * MOMENTS * MOMENTS * rows
    rest = acc[...].reshape(count, LANES)
    ones = jnp.ones((SUBS, LANES), jnp.bfloat16)
    total = None
    for _ in range(3):
        piece = rest.astype(jnp.bfloat16)
        rest = rest - piece.astype(jnp.float32)
        part = lax.dot_general(
            ones, piece, (((1,), (1,)), ((), ())), preferred_element_type=jnp.float32
        )
        total = part if total is None else total + part

    row8 = jnp.where(sub8 < 4, jnp.where(sub8 == 2, 1, 0), jnp.where(sub8 == 6, rows - 2, rows - 1))
    row8 = jnp.where((sub8 == 0) | (sub8 == 4), -LANES, row8)
    per = LANES // rows
    for j in range(0, 2 * MOMENTS * MOMENTS, per):
        chosen = each_sum()[j : j + per]
        piece = jnp.zeros((SUBS, LANES), jnp.float32)
        for k, (p, n, m) in enumerate(chosen):
            value = jnp.sum(found[p][n][m], axis=1, keepdims=True)
            piece = jnp.where(lane8 == row8 + k * rows, value * SIXTH if m == 1 else value, piece)
        for step in (4, 2, 1):
            piece = piece + pltpu.roll(piece, step, 0)
        span = slice(j * rows, (j + len(chosen)) * rows)
        part_mom[0, :, span] = total[:, span] + piece[:, 0 : len(chosen) * rows]

    swaps = []
    for d in range(1, gyn):
        copy = pltpu.make_async_remote_copy(
            src_ref=part_mom.at[0, 0:1], dst_ref=part_mom.at[d, 0:1],
            send_sem=msend_sem.at[d - 1], recv_sem=mrecv_sem.at[d - 1],
            device_id=peer(0, d), device_id_type=MESH,
        )
        copy.start()
        swaps.append(copy)

    def patch(v, carry):
        turn_first = lax.rem(2 * LANES - GROUP // 2 - GROUP * v, LANES)
        turn_last = lax.rem(2 * LANES - GROUP // 2 + HALF - GROUP * v, LANES)
        for p in range(2):
            for sub in range(2):
                for s, buf in ((2, lbuf), (4, rbuf)):
                    side = cv[s, p, sub]
                    for t in range(tiles):
                        value = buf[v, 1 - p, sub, :, tile(t)].astype(jnp.float32)
                        over = bw[v, p, s, :, tile(t)]
                        edge = -side if p == 0 else side
                        over = -over if p == 0 else over
                        top = jnp.where(
                            sub8 < EDGE - sub, pltpu.roll(over, SUBS - 1 - 2 * sub, 0), value[0:SUBS]
                        )
                        bottom = jnp.where(
                            sub8 >= SUBS - 1 - sub, over if sub else pltpu.roll(over, 2, 0), value[rows - SUBS : rows]
                        )
                        value = jnp.concatenate([top, value[SUBS : rows - SUBS], bottom] if rows > 2 * SUBS else [top, bottom], 0)
                        if t == 0:
                            value = jnp.where(lane_r < EDGE, pltpu.roll(edge, turn_first, 1), value)
                        if t == last:
                            value = jnp.where(lane_r >= LANES - EDGE, pltpu.roll(edge, turn_last, 1), value)
                        buf[v, 1 - p, sub, :, tile(t)] = value.astype(jnp.bfloat16)
        return carry

    lax.fori_loop(0, vectors, patch, 0)

    for copy in swaps:
        copy.wait_recv()
    total = part_mom[0]
    for d in range(1, gyn):
        total = total + part_mom[d]
    out_mom[...] = total / float(vectors * cols * gyn)
    for copy in sends + swaps:
        copy.wait_send()


def writer(total, lbuf, rbuf, out_mom, out_left, out_right, mom, out_sem):
    outs = [
        pltpu.make_async_copy(lbuf, out_left, out_sem.at[0]),
        pltpu.make_async_copy(rbuf, out_right, out_sem.at[1]),
    ]
    for copy in outs:
        copy.start()
    rows = mom.shape[3]
    for p in range(2):
        for n in range(MOMENTS):
            for m in range(MOMENTS):
                k = (p * MOMENTS + n) * MOMENTS + m
                mom[n, m, p : p + 1, :] = total[0:1, k * rows : (k + 1) * rows]
    outs.append(pltpu.make_async_copy(mom, out_mom, out_sem.at[2]))
    outs[2].start()
    for copy in outs:
        copy.wait()


def solution(mesh):
    gxn, gyn = mesh.shape["gx"], mesh.shape["gy"]

    def per_device(vectors, bonds, onsite):
        count, _, _, rows, cols = vectors.shape
        tall = rows + 8
        f32 = jnp.float32
        in_hbm = pl.BlockSpec(memory_space=pltpu.HBM)
        last = jax.ShapeDtypeStruct(vectors.shape, jnp.bfloat16)
        sends = 16
        in_vmem = pl.BlockSpec(memory_space=pltpu.VMEM)
        sums = (8, 2 * MOMENTS * MOMENTS * rows)
        made = pl.pallas_call(
            functools.partial(kernel, gxn, gyn),
            out_shape=(
                pltpu.VMEM(sums, f32),
                pltpu.VMEM(vectors.shape, jnp.bfloat16),
                pltpu.VMEM(vectors.shape, jnp.bfloat16),
            ),
            in_specs=[in_hbm] * 3,
            out_specs=(in_vmem,) * 3,
            scratch_shapes=[
                pltpu.VMEM(vectors.shape, f32),
                pltpu.VMEM((count, 2, 2, SUBS, cols), f32),
                pltpu.VMEM((5, rows, cols), f32),
                pltpu.VMEM((5, SUBS, cols), f32),
                pltpu.VMEM((5, SUBS, cols), f32),
                pltpu.VMEM((count, 2, 2, SUBS, cols), f32),
                pltpu.VMEM((4, 7, rows, cols), f32),
                pltpu.VMEM((4, 7, SUBS, cols), f32),
                pltpu.VMEM((5, SUBS, LANES), f32),
                pltpu.VMEM((5, tall, LANES), f32),
                pltpu.VMEM((5, tall, LANES), f32),
                pltpu.VMEM((5, tall, LANES), f32),
                pltpu.VMEM((7, tall, LANES), f32),
                pltpu.VMEM((SLOTS, 2, 2, rows, LANES), f32),
                pltpu.VMEM((count, 2, SLOTS, SUBS, cols), f32),
                pltpu.VMEM((count, 2, 3, 2, SUBS, cols), f32),
                pltpu.VMEM((4, count, 2, 2, SUBS, cols), f32),
                pltpu.VMEM((SLOTS, 2, 2, rows, cols), f32),
                pltpu.VMEM((2, MOMENTS, MOMENTS, rows, LANES), f32),
                pltpu.VMEM((gyn, *sums), f32),
                pltpu.SemaphoreType.DMA((5,)),
                pltpu.SemaphoreType.DMA((sends,)),
                pltpu.SemaphoreType.DMA((sends,)),
                pltpu.SemaphoreType.DMA((gyn - 1,)),
                pltpu.SemaphoreType.DMA((gyn - 1,)),
            ],
            compiler_params=pltpu.CompilerParams(
                collective_id=0, has_side_effects=True, vmem_limit_bytes=GRANT
            ),
        )(*(pltpu.with_memory_space_constraint(array, pltpu.HBM) for array in (vectors, bonds, onsite)))
        made = [pltpu.with_memory_space_constraint(array, pltpu.VMEM) for array in made]
        moments, left, right = pl.pallas_call(
            writer,
            out_shape=(
                jax.ShapeDtypeStruct((MOMENTS, MOMENTS, 2, rows), f32), last, last,
            ),
            in_specs=[in_vmem] * 3,
            out_specs=(in_hbm,) * 3,
            scratch_shapes=[
                pltpu.VMEM((MOMENTS, MOMENTS, 2, rows), f32),
                pltpu.SemaphoreType.DMA((3,)),
            ],
            compiler_params=pltpu.CompilerParams(vmem_limit_bytes=GRANT),
        )(*made)
        return jnp.transpose(moments, (2, 0, 1, 3)), left, right

    return jax.shard_map(
        per_device,
        mesh=mesh,
        in_specs=(P(None, None, None, "gx", "gy"), P(None, "gx", "gy"), P(None, "gx", "gy")),
        out_specs=(
            P(None, None, None, "gx"),
            P(None, None, None, "gx", "gy"),
            P(None, None, None, "gx", "gy"),
        ),
        check_vma=False,
    )
```

```python
import functools
import jax
import jax.numpy as jnp
from jax import lax
from jax.experimental import pallas as pl
from jax.experimental.pallas import tpu as pltpu
from jax.sharding import PartitionSpec as P

MOMENTS = 3
SCALE = 6.0
EDGE = 2
GROUP = 8
HALF = 64
LANES = 128
SUBS = 8
SLOTS = 5
GRANT = 32 * 1024 * 1024
MESH = pl.DeviceIdType.MESH
SIXTH = 1.0 / SCALE
HALF_SQUARE = 0.5 * SCALE * SCALE
BENT_INNER = (2.0, -1.0, -1.0, -1.0, -1.0)
BENT_WINDOW = (2.0, -1.0, -1.0, 2.0, -1.0)


def tile(t):
    return slice(t * LANES, (t + 1) * LANES)


def up(t):
    return pltpu.roll(t, 1, 0)


def down(t):
    return pltpu.roll(t, t.shape[0] - 1, 0)


def speed(terms):
    a0, a12, b0, b12 = terms
    return a0 - 0.5 * a12, 0.5 * b12 - b0


def energy(pair, terms, on, factor=None):
    a0, a12, b0, b12 = terms
    a, b = on[0] * pair[0] + (a0 + a12), on[1] * pair[1] + (b0 + b12)
    return (a, b) if factor is None else (a * factor, b * factor)


def add_products(sums, left, right):
    for n in range(MOMENTS):
        for m in range(MOMENTS):
            (p, q), (r, s) = left[n], right[m]
            sums[0][n][m] = sums[0][n][m] + (p * r + q * s)
            sums[1][n][m] = sums[1][n][m] + (p * s - q * r)


def rights_of(at):
    return [at[0], at[3], at[4]]


def masked(mask, at):
    return [[jnp.where(mask, item, 0.0) for item in at[n]] for n in range(MOMENTS)]


def each_sum():
    return [(p, n, m) for p in range(2) for n in range(MOMENTS) for m in range(MOMENTS)]


def kernel(
    gxn, gyn, vec, bonds, onsite, out_mom, lbuf, rbuf,
    x, xe, f, fw, fo, hw, gb, gw, cc, cs, ms, c_own, c_left, c_right, hf, cv, bw, lk, state, keep, acc, part_mom,
    load_sem, send_sem, recv_sem, msend_sem, mrecv_sem,
):
    vectors, _, _, rows, cols = vec.shape
    tall = c_own.shape[1]
    tiles = cols // LANES
    last = tiles - 1
    gx = lax.axis_index("gx")
    gy = lax.axis_index("gy")

    def peer(dx, dy):
        return (lax.rem(gx + dx + gxn, gxn), lax.rem(gy + dy + gyn, gyn))

    barrier = pltpu.get_barrier_semaphore()
    near = [(dx % gxn, dy % gyn) for dx in (-1, 1) for dy in (0, 1, -1)]
    near += [(0, dy) for dy in range(gyn)]
    near = [one for k, one in enumerate(near) if one != (0, 0) and one not in near[:k]]
    for dx, dy in near:
        pl.semaphore_signal(barrier, inc=1, device_id=peer(dx, dy), device_id_type=MESH)

    low, high = slice(0, EDGE), slice(SUBS - EDGE, SUBS)
    loads = [
        pltpu.make_async_copy(vec.at[:, :, :, 0:EDGE, :], xe.at[:, :, :, low, :], load_sem.at[0]),
        pltpu.make_async_copy(
            vec.at[:, :, :, rows - EDGE : rows, :], xe.at[:, :, :, high, :], load_sem.at[1]
        ),
        pltpu.make_async_copy(bonds, f.at[0:3], load_sem.at[2]),
        pltpu.make_async_copy(onsite, f.at[3:5], load_sem.at[3]),
        pltpu.make_async_copy(vec, x, load_sem.at[4]),
    ]
    for copy in loads:
        copy.start()

    hw[:, :, 0, 1 : SUBS - EDGE, :] = jnp.zeros((vectors, 2, SUBS - EDGE - 1, cols), jnp.float32)
    hw[:, :, 1, EDGE : SUBS - 1, :] = jnp.zeros((vectors, 2, SUBS - EDGE - 1, cols), jnp.float32)
    acc[...] = jnp.zeros_like(acc)
    sends = []

    def send(src, dst, dx, dy):
        n = len(sends)
        copy = pltpu.make_async_remote_copy(
            src_ref=src, dst_ref=dst, send_sem=send_sem.at[n], recv_sem=recv_sem.at[n],
            device_id=peer(dx, dy), device_id_type=MESH,
        )
        sends.append(copy)
        return copy

    def packed(items):
        count = items[0][0].shape[0]
        lane = lax.broadcasted_iota(jnp.int32, (count, LANES), 1)
        spot = lax.rem(lane, HALF)
        total = None
        for k, (first, final) in enumerate(items):
            both = jnp.where(lane < HALF, first, final)
            place = lax.rem(spot + (2 * LANES - GROUP * k - GROUP // 2), LANES)
            moved = jnp.take_along_axis(both, place, axis=1)
            total = jnp.where(spot // GROUP == k, moved, total) if k else moved
        return total

    def sides_of(four):
        lane = lax.broadcasted_iota(jnp.int32, four[0].shape, 1)
        start = lane + jnp.where(lane < HALF, 2, 4)
        spot = lax.rem(lane, GROUP)
        total = None
        for k, one in enumerate(four):
            moved = jnp.take_along_axis(one, lax.rem(start + (LANES - 2 * k), LANES), axis=1)
            total = jnp.where(spot // 2 == k, moved, total) if k else moved
        return total

    def ends(ref, *index):
        return ref[(*index, slice(None), slice(0, LANES))], ref[
            (*index, slice(None), slice(cols - LANES, cols))
        ]

    sub8 = lax.broadcasted_iota(jnp.int32, (SUBS, LANES), 0)
    lane8 = lax.broadcasted_iota(jnp.int32, (SUBS, LANES), 1)

    def window_a(t):
        return jnp.where(
            sub8 < 4, pltpu.roll(t[0:SUBS], 1, 0), pltpu.roll(t[rows - SUBS : rows], SUBS - 2, 0)
        )

    def window_b(t):
        return jnp.where(
            sub8 < 4, pltpu.roll(t[0:SUBS], 2, 0), pltpu.roll(t[rows - SUBS : rows], SUBS - 1, 0)
        )

    for copy in loads[:4]:
        copy.wait()
    for p in range(2):
        for sub in range(2):
            cc[2 * p + sub] = packed([ends(xe, v, p, sub) for v in range(vectors)])
    cs[0] = sides_of([cc[k] for k in range(4)])

    def rim_rows(t):
        return jnp.where(sub8 < 4, t[0:SUBS], t[rows - SUBS : rows])

    cc[4] = packed([tuple(rim_rows(t) for t in ends(f, k)) for k in range(5)])
    cs[1] = cc[4]
    lane_r = lax.broadcasted_iota(jnp.int32, (rows, LANES), 1)
    core = slice(0, rows)

    def pack_block():
        loads[4].wait()
        for p in range(2):
            for sub in range(2):
                c_own[2 * p + sub, core] = packed([ends(x, v, p, sub) for v in range(vectors)])
        c_own[4, core] = packed([ends(f, k) for k in range(5)])
        ms[0] = sides_of([c_own[k, core] for k in range(4)])
        ms[1] = c_own[4, core]

    def fill(g, bent, fields, t):
        for i, item in enumerate(fields):
            g[3, i, :, tile(t)] = item
            g[0, i, :, tile(t)] = item * SIXTH
            g[1, i, :, tile(t)] = item * (2.0 * SIXTH)
            if i < 5:
                g[2, i, :, tile(t)] = item * (bent[i] * SIXTH * SIXTH)

    def turned(items, shift):
        size = items[0].shape
        lane = lax.broadcasted_iota(jnp.int32, size, 1)
        rolled = [pltpu.roll(t, shift % LANES, 1) for t in items]
        if shift > 0:
            return rolled[:1] + [jnp.where(lane == 0, rolled[t - 1], rolled[t]) for t in range(1, tiles)]
        return [
            jnp.where(lane == LANES - 1, rolled[t + 1], rolled[t]) for t in range(last)
        ] + rolled[last:]

    def inner_terms(a, b, w):
        left, right = turned(b, 1), turned(a, -1)
        found = []
        for t in range(tiles):
            f0, f1, f2, d1, d2 = (gb[w, i, :, tile(t)] for i in range(5))
            found.append((f0 * b[t], f1 * up(b[t]) + f2 * left[t], f0 * a[t], d1 * down(a[t]) + d2 * right[t]))
        return found

    def window_terms(a, b, w, leak=None):
        b_up, a_down = [down(t) for t in b], [up(t) for t in a]
        left, right = turned(b_up, 1), turned(a_down, -1)
        found = []
        for t in range(tiles):
            f0, f1, f2, d0, d2 = (gw[w, i, :, tile(t)] for i in range(5))
            over_a = a[t] if leak is None else a[t] + leak[0][t]
            over_b = b[t] if leak is None else b[t] + leak[1][t]
            found.append((f0 * b_up[t], f1 * over_b + f2 * left[t], d0 * a_down[t], f1 * over_a + d2 * right[t]))
        return found

    def both(items):
        return [item[0] for item in items], [item[1] for item in items]

    def at_tile(pair, t):
        return pair[0][t], pair[1][t]

    def chains(q0, terms, g, leaks):
        def on(w, t):
            return g[w, 5, :, tile(t)], g[w, 6, :, tile(t)]

        def less(pair, other, times=None):
            return both(
                [
                    tuple(
                        one - (two if times is None else two * times)
                        for one, two in zip(at_tile(pair, t), at_tile(other, t))
                    )
                    for t in range(tiles)
                ]
            )

        def stepped(pair, found, w):
            return both([energy(at_tile(pair, t), found[t], on(w, t)) for t in range(tiles)])

        t0 = terms(*q0, 3, *leaks[0:1])
        m0 = both([speed(item) for item in t0])
        q1 = stepped(q0, t0, 3)
        t1 = terms(*q1, 3, *leaks[1:2])
        n1 = both([speed(item) for item in t1])
        q2 = less(stepped(q1, t1, 3), q0, HALF_SQUARE)
        n2 = both([(a0 + a12, -(b0 + b12)) for a0, a12, b0, b12 in terms(*q2, 2)])
        m1 = stepped(m0, terms(*m0, 0, *leaks[2:3]), 0)
        m2 = less(stepped(m1, terms(*m1, 1), 1), m0)
        return q1, (m0, m1, m2, n1, n2)

    def inside_lanes(t):
        keep_lanes = None
        if t == 0:
            keep_lanes = lane8 >= EDGE
        if t == last:
            end = lane8 < LANES - EDGE
            keep_lanes = end if keep_lanes is None else keep_lanes & end
        return keep_lanes

    def inside(sub, r, t):
        keep_cells = inside_lanes(t)
        cuts = []
        if r == 0:
            cuts.append(sub8 >= EDGE - sub)
        if r == rows - SUBS:
            cuts.append(sub8 < SUBS - 1 - sub)
        for one in cuts:
            keep_cells = one if keep_cells is None else keep_cells & one
        return keep_cells

    def one_vector(v, carry):
        for p in range(2):
            q0 = tuple([x[v, p, sub, :, tile(t)] for t in range(tiles)] for sub in range(2))
            q1, slots = chains(q0, inner_terms, gb, ())
            for s, pair in enumerate(slots):
                for t in range(tiles):
                    for sub in range(2):
                        keep[s, p, sub, :, tile(t)] = pair[sub][t]
                    a, b = pair[0][t], pair[1][t]
                    ends_a, ends_b = (a[0:SUBS], a[rows - SUBS : rows]), (b[0:SUBS], b[rows - SUBS : rows])
                    over = jnp.where(sub8 == 3, pltpu.roll(ends_b[0], 3, 0), ends_b[1])
                    over = jnp.where(sub8 == 5, pltpu.roll(ends_a[1], SUBS - 2, 0), over)
                    bw[v, p, s, :, tile(t)] = jnp.where(
                        (sub8 == 1) | (sub8 == 2), pltpu.roll(ends_a[0], 1, 0), over
                    )
            for s, pair in enumerate((q0, q1, slots[0])):
                for t in range(tiles):
                    lk[v, p, s, 0, :, tile(t)] = jnp.where(sub8 == 1, window_a(pair[0][t]), 0.0)
                    lk[v, p, s, 1, :, tile(t)] = jnp.where(sub8 == 6, window_b(pair[1][t]), 0.0)
            for buf, pair in ((lbuf, slots[2]), (rbuf, slots[4])):
                for sub in range(2):
                    for t in range(tiles):
                        value = -pair[sub][t] if p == 0 else pair[sub][t]
                        buf[v, 1 - p, sub, :, tile(t)] = value.astype(jnp.bfloat16)

        for r in range(0, rows, SUBS):
            band = slice(r, r + SUBS)
            sums = [[[acc[p, n, m, band, :] for m in range(MOMENTS)] for n in range(MOMENTS)] for p in range(2)]
            for sub in range(2):
                for t in range(tiles):
                    at = [[keep[s, p, sub, band, tile(t)] for p in range(2)] for s in range(SLOTS)]
                    mask = inside(sub, r, t)
                    add_products(sums, at[:MOMENTS] if mask is None else masked(mask, at), rights_of(at))
            for p, n, m in each_sum():
                acc[p, n, m, band, :] = sums[p][n][m]
        return carry

    def own_block():
        sub_r = lax.broadcasted_iota(jnp.int32, (rows, LANES), 0)
        shifted = turned([f[2, :, tile(t)] for t in range(tiles)], -1)
        for t in range(tiles):
            inner = jnp.where(sub_r == 0, 0.0, f[1, :, tile(t)])
            fill(
                gb,
                BENT_INNER,
                (f[0, :, tile(t)], inner, f[2, :, tile(t)], down(inner), shifted[t],
                 f[3, :, tile(t)], f[4, :, tile(t)]),
                t,
            )
            for k in range(4):
                fo[k, :, tile(t)] = window_a(f[k, :, tile(t)])
            fo[4, :, tile(t)] = window_b(f[4, :, tile(t)])
        lax.fori_loop(0, vectors, one_vector, 0)

    early = gx == 0

    @pl.when(early)
    def _():
        pack_block()
        own_block()

    pl.semaphore_wait(barrier, len(near))

    past, ahead = slice(rows, rows + EDGE), slice(tall - EDGE, tall)
    sides = [
        send(ms, c_right.at[:, core, :], 0, -1),
        send(ms, c_left.at[:, core, :], 0, 1),
    ]
    rims = [
        send(f.at[0:4, rows - 1 : rows, :], fw.at[0:4, 0:1, :], 1, 0),
        send(f.at[4:5, rows - 2 : rows, :], fw.at[4:5, 0:2, :], 1, 0),
    ]
    for src, dst, dy in ((cs, c_right, -1), (cs, c_left, 1), (cc, c_own, 0)):
        rims.append(send(src.at[:, high, :], dst.at[:, ahead, :], 1, dy))
    rims += [
        send(xe.at[:, :, 1, SUBS - 2 : SUBS, :], hw.at[:, :, 1, 0:2, :], 1, 0),
        send(xe.at[:, :, 0, SUBS - 1 : SUBS, :], hw.at[:, :, 0, 0:1, :], 1, 0),
        send(f.at[0:4, 0:2, :], fw.at[0:4, SUBS - 2 : SUBS, :], -1, 0),
        send(f.at[4:5, 0:1, :], fw.at[4:5, SUBS - 1 : SUBS, :], -1, 0),
    ]
    for src, dst, dy in ((cs, c_right, -1), (cs, c_left, 1), (cc, c_own, 0)):
        rims.append(send(src.at[:, low, :], dst.at[:, past, :], -1, dy))
    rims += [
        send(xe.at[:, :, 0, 0:2, :], hw.at[:, :, 0, SUBS - 2 : SUBS, :], -1, 0),
        send(xe.at[:, :, 1, 0:1, :], hw.at[:, :, 1, SUBS - 1 : SUBS, :], -1, 0),
    ]

    @pl.when(early)
    def _():
        for copy in sides:
            copy.start()

    for copy in rims:
        copy.start()

    @pl.when(jnp.logical_not(early))
    def _():
        pack_block()
        for copy in sides:
            copy.start()
        own_block()

    row_sends = rims[5:7] + rims[12:14]
    for copy in sides + rims[0:5] + rims[7:12]:
        copy.wait_recv()

    taken_a = (sub8 < 1) | (sub8 >= SUBS - 2)
    taken_b = (sub8 < 2) | (sub8 >= SUBS - 1)
    cut = (sub8 == 3) | (sub8 == SUBS - 1)
    windows = [
        [jnp.where(taken_b if k == 4 else taken_a, fw[k, :, tile(t)], fo[k, :, tile(t)]) for t in range(tiles)]
        for k in range(5)
    ]
    for k in (0, 2):
        windows[k] = [jnp.where(cut, 0.0, t) for t in windows[k]]
    far = turned([up(t) for t in windows[2]], -1)
    for t in range(tiles):
        fill(
            gw,
            BENT_WINDOW,
            (windows[0][t], windows[1][t], windows[2][t], up(windows[0][t]), far[t], windows[3][t], windows[4][t]),
            t,
        )


    tlane = lax.broadcasted_iota(jnp.int32, (tall, LANES), 1)
    tspot = lax.rem(tlane, GROUP)
    on_left = tlane < HALF
    from_side = jnp.where(on_left, tspot, tspot - 2) // 2 == 1
    side = jnp.where(on_left, c_left[0], c_right[0])
    side_start = tlane + jnp.where(on_left, LANES - 2, LANES - 4)

    def joined(k):
        moved = jnp.take_along_axis(side, lax.rem(side_start + 2 * k, LANES), axis=1)
        return jnp.where(from_side, moved, c_own[k])

    field_tile = jnp.where(from_side, jnp.where(on_left, c_left[1], c_right[1]), c_own[4])
    place = (tlane // HALF) * HALF + tspot
    for k in range(5):
        hf[k] = jnp.take_along_axis(field_tile, place + GROUP * k, axis=1)
    hf[5] = down(hf[1])
    hf[6] = jnp.take_along_axis(field_tile, lax.rem(place + (2 * GROUP + 1), LANES), axis=1)
    h_on = (hf[3], hf[4])

    def rim_terms(a, b):
        f0, f1, f2, d1, d2 = hf[0], hf[1], hf[2], hf[5], hf[6]
        return (
            f0 * b, f1 * up(b) + f2 * pltpu.roll(b, 1, 1),
            f0 * a, d1 * down(a) + d2 * pltpu.roll(a, LANES - 1, 1),
        )

    for p in range(2):
        q0 = (joined(2 * p), joined(2 * p + 1))
        t0 = rim_terms(*q0)
        m0 = speed(t0)
        q1 = energy(q0, t0, h_on)
        t1 = rim_terms(*q1)
        n1 = speed(t1)
        h1 = energy(q1, t1, h_on)
        q2 = (h1[0] - HALF_SQUARE * q0[0], h1[1] - HALF_SQUARE * q0[1])
        n2 = tuple(item / HALF_SQUARE for item in speed(rim_terms(*q2)))
        m1 = energy(m0, rim_terms(*m0), h_on, SIXTH)
        h2 = energy(m1, rim_terms(*m1), h_on, 2.0 * SIXTH)
        m2 = (h2[0] - m0[0], h2[1] - m0[1])
        for s, pair in enumerate((m0, m1, m2, n1, n2)):
            for sub in range(2):
                cv[s, p, sub] = pair[sub][0:rows]

    spot8 = lax.rem(lane8, GROUP)
    rim_lanes = ((lane8 < HALF) & ((spot8 == 4) | (spot8 == 5))) | (
        (lane8 >= HALF) & ((spot8 == 2) | (spot8 == 3))
    )


    def none():
        zero = jnp.zeros((SUBS, LANES), jnp.float32)
        return [[[zero for _ in range(MOMENTS)] for _ in range(MOMENTS)] for _ in range(2)]

    for r in range(0, rows, SUBS):
        band = slice(r, r + SUBS)
        sums = none()
        for sub in range(2):
            at = [[cv[s, p, sub, band] for p in range(2)] for s in range(SLOTS)]
            add_products(sums, masked(rim_lanes, at), rights_of(at))
        for p, n, m in each_sum():
            value = acc[p, n, m, band, :] + sums[p][n][m]
            acc[p, n, m, band, :] = value * SIXTH if m == 1 else value

    count = 2 * MOMENTS * MOMENTS * rows
    rest = acc[...].reshape(count, LANES)
    ones = jnp.ones((SUBS, LANES), jnp.bfloat16)
    total = None
    for _ in range(3):
        piece = rest.astype(jnp.bfloat16)
        rest = rest - piece.astype(jnp.float32)
        part = lax.dot_general(
            ones, piece, (((1,), (1,)), ((), ())), preferred_element_type=jnp.float32
        )
        total = part if total is None else total + part

    for copy in row_sends:
        copy.wait_recv()

    from_a = (sub8 == 1) | (sub8 == 2) | (sub8 == 5)
    planes = [(v, p) for v in range(vectors) for p in range(2)]

    def pair_of(ref, *index):
        return tuple([ref[(*index, sub, slice(None), tile(t))] for t in range(tiles)] for sub in range(2))

    def on_window(pair, found, w):
        return both(
            [
                energy(at_tile(pair, t), found[t], (gw[w, 5, :, tile(t)], gw[w, 6, :, tile(t)]))
                for t in range(tiles)
            ]
        )

    def put(k, v, p, pair):
        for sub in range(2):
            for t in range(tiles):
                state[k, v, p, sub, :, tile(t)] = pair[sub][t]

    def add(v, p, s, pair):
        for t in range(tiles):
            change = jnp.where(from_a, pair[0][t], up(pair[1][t]))
            bw[v, p, s, :, tile(t)] = bw[v, p, s, :, tile(t)] + change

    def minus(pair, other, times=None):
        return tuple(
            [one - (two if times is None else two * times) for one, two in zip(pair[sub], other[sub])]
            for sub in range(2)
        )

    for v, p in planes:
        pair = pair_of(hw, v, p)
        found = window_terms(*pair, 3, pair_of(lk, v, p, 0))
        m0 = both([speed(item) for item in found])
        put(0, v, p, on_window(pair, found, 3))
        put(1, v, p, m0)
        add(v, p, 0, m0)
    for v, p in planes:
        pair = pair_of(state, 0, v, p)
        found = window_terms(*pair, 3, pair_of(lk, v, p, 1))
        add(v, p, 3, both([speed(item) for item in found]))
        put(2, v, p, minus(on_window(pair, found, 3), pair_of(hw, v, p), HALF_SQUARE))
    for v, p in planes:
        pair = pair_of(state, 1, v, p)
        m1 = on_window(pair, window_terms(*pair, 0, pair_of(lk, v, p, 2)), 0)
        put(3, v, p, m1)
        add(v, p, 1, m1)
    for v, p in planes:
        found = window_terms(*pair_of(state, 2, v, p), 2)
        add(v, p, 4, both([(a0 + a12, -(b0 + b12)) for a0, a12, b0, b12 in found]))
    for v, p in planes:
        pair = pair_of(state, 3, v, p)
        add(v, p, 2, minus(on_window(pair, window_terms(*pair, 1), 1), pair_of(state, 1, v, p)))

    found = none()
    for t in range(tiles):
        sums = none()
        for v in range(vectors):
            at = [[bw[v, p, s, :, tile(t)] for p in range(2)] for s in range(SLOTS)]
            add_products(sums, at[:MOMENTS], rights_of(at))
        mask = inside_lanes(t)
        for p, n, m in each_sum():
            value = sums[p][n][m] if mask is None else jnp.where(mask, sums[p][n][m], 0.0)
            found[p][n][m] = value if t == 0 else found[p][n][m] + value
    row8 = jnp.where(sub8 < 4, jnp.where(sub8 == 2, 1, 0), jnp.where(sub8 == 6, rows - 2, rows - 1))
    row8 = jnp.where((sub8 == 0) | (sub8 == 4), -LANES, row8)
    per = LANES // rows
    for j in range(0, 2 * MOMENTS * MOMENTS, per):
        chosen = each_sum()[j : j + per]
        piece = jnp.zeros((SUBS, LANES), jnp.float32)
        for k, (p, n, m) in enumerate(chosen):
            value = jnp.sum(found[p][n][m], axis=1, keepdims=True)
            piece = jnp.where(lane8 == row8 + k * rows, value * SIXTH if m == 1 else value, piece)
        for step in (4, 2, 1):
            piece = piece + pltpu.roll(piece, step, 0)
        span = slice(j * rows, (j + len(chosen)) * rows)
        part_mom[0, :, span] = total[:, span] + piece[:, 0 : len(chosen) * rows]

    swaps = []
    for d in range(1, gyn):
        copy = pltpu.make_async_remote_copy(
            src_ref=part_mom.at[0, 0:1], dst_ref=part_mom.at[d, 0:1],
            send_sem=msend_sem.at[d - 1], recv_sem=mrecv_sem.at[d - 1],
            device_id=peer(0, d), device_id_type=MESH,
        )
        copy.start()
        swaps.append(copy)

    def patch(v, carry):
        turn_first = lax.rem(2 * LANES - GROUP // 2 - GROUP * v, LANES)
        turn_last = lax.rem(2 * LANES - GROUP // 2 + HALF - GROUP * v, LANES)
        for p in range(2):
            for sub in range(2):
                for s, buf in ((2, lbuf), (4, rbuf)):
                    side = cv[s, p, sub]
                    for t in range(tiles):
                        value = buf[v, 1 - p, sub, :, tile(t)].astype(jnp.float32)
                        over = bw[v, p, s, :, tile(t)]
                        edge = -side if p == 0 else side
                        over = -over if p == 0 else over
                        top = jnp.where(
                            sub8 < EDGE - sub, pltpu.roll(over, SUBS - 1 - 2 * sub, 0), value[0:SUBS]
                        )
                        bottom = jnp.where(
                            sub8 >= SUBS - 1 - sub, over if sub else pltpu.roll(over, 2, 0), value[rows - SUBS : rows]
                        )
                        value = jnp.concatenate([top, value[SUBS : rows - SUBS], bottom] if rows > 2 * SUBS else [top, bottom], 0)
                        if t == 0:
                            value = jnp.where(lane_r < EDGE, pltpu.roll(edge, turn_first, 1), value)
                        if t == last:
                            value = jnp.where(lane_r >= LANES - EDGE, pltpu.roll(edge, turn_last, 1), value)
                        buf[v, 1 - p, sub, :, tile(t)] = value.astype(jnp.bfloat16)
        return carry

    lax.fori_loop(0, vectors, patch, 0)

    for copy in swaps:
        copy.wait_recv()
    total = part_mom[0]
    for d in range(1, gyn):
        total = total + part_mom[d]
    out_mom[...] = total / float(vectors * cols * gyn)
    for copy in sends + swaps:
        copy.wait_send()


def writer(total, lbuf, rbuf, out_mom, out_left, out_right, mom, out_sem):
    outs = [
        pltpu.make_async_copy(lbuf, out_left, out_sem.at[0]),
        pltpu.make_async_copy(rbuf, out_right, out_sem.at[1]),
    ]
    for copy in outs:
        copy.start()
    rows = mom.shape[3]
    for p in range(2):
        for n in range(MOMENTS):
            for m in range(MOMENTS):
                k = (p * MOMENTS + n) * MOMENTS + m
                mom[n, m, p : p + 1, :] = total[0:1, k * rows : (k + 1) * rows]
    outs.append(pltpu.make_async_copy(mom, out_mom, out_sem.at[2]))
    outs[2].start()
    for copy in outs:
        copy.wait()


def solution(mesh):
    gxn, gyn = mesh.shape["gx"], mesh.shape["gy"]

    def per_device(vectors, bonds, onsite):
        count, _, _, rows, cols = vectors.shape
        tall = rows + 8
        f32 = jnp.float32
        in_hbm = pl.BlockSpec(memory_space=pltpu.HBM)
        last = jax.ShapeDtypeStruct(vectors.shape, jnp.bfloat16)
        sends = 16
        in_vmem = pl.BlockSpec(memory_space=pltpu.VMEM)
        sums = (8, 2 * MOMENTS * MOMENTS * rows)
        made = pl.pallas_call(
            functools.partial(kernel, gxn, gyn),
            out_shape=(
                pltpu.VMEM(sums, f32),
                pltpu.VMEM(vectors.shape, jnp.bfloat16),
                pltpu.VMEM(vectors.shape, jnp.bfloat16),
            ),
            in_specs=[in_hbm] * 3,
            out_specs=(in_vmem,) * 3,
            scratch_shapes=[
                pltpu.VMEM(vectors.shape, f32),
                pltpu.VMEM((count, 2, 2, SUBS, cols), f32),
                pltpu.VMEM((5, rows, cols), f32),
                pltpu.VMEM((5, SUBS, cols), f32),
                pltpu.VMEM((5, SUBS, cols), f32),
                pltpu.VMEM((count, 2, 2, SUBS, cols), f32),
                pltpu.VMEM((4, 7, rows, cols), f32),
                pltpu.VMEM((4, 7, SUBS, cols), f32),
                pltpu.VMEM((5, SUBS, LANES), f32),
                pltpu.VMEM((2, SUBS, LANES), f32),
                pltpu.VMEM((2, rows, LANES), f32),
                pltpu.VMEM((5, tall, LANES), f32),
                pltpu.VMEM((2, tall, LANES), f32),
                pltpu.VMEM((2, tall, LANES), f32),
                pltpu.VMEM((7, tall, LANES), f32),
                pltpu.VMEM((SLOTS, 2, 2, rows, LANES), f32),
                pltpu.VMEM((count, 2, SLOTS, SUBS, cols), f32),
                pltpu.VMEM((count, 2, 3, 2, SUBS, cols), f32),
                pltpu.VMEM((4, count, 2, 2, SUBS, cols), f32),
                pltpu.VMEM((SLOTS, 2, 2, rows, cols), f32),
                pltpu.VMEM((2, MOMENTS, MOMENTS, rows, LANES), f32),
                pltpu.VMEM((gyn, *sums), f32),
                pltpu.SemaphoreType.DMA((5,)),
                pltpu.SemaphoreType.DMA((sends,)),
                pltpu.SemaphoreType.DMA((sends,)),
                pltpu.SemaphoreType.DMA((gyn - 1,)),
                pltpu.SemaphoreType.DMA((gyn - 1,)),
            ],
            compiler_params=pltpu.CompilerParams(
                collective_id=0, has_side_effects=True, vmem_limit_bytes=GRANT
            ),
        )(*(pltpu.with_memory_space_constraint(array, pltpu.HBM) for array in (vectors, bonds, onsite)))
        made = [pltpu.with_memory_space_constraint(array, pltpu.VMEM) for array in made]
        moments, left, right = pl.pallas_call(
            writer,
            out_shape=(
                jax.ShapeDtypeStruct((MOMENTS, MOMENTS, 2, rows), f32), last, last,
            ),
            in_specs=[in_vmem] * 3,
            out_specs=(in_hbm,) * 3,
            scratch_shapes=[
                pltpu.VMEM((MOMENTS, MOMENTS, 2, rows), f32),
                pltpu.SemaphoreType.DMA((3,)),
            ],
            compiler_params=pltpu.CompilerParams(vmem_limit_bytes=GRANT),
        )(*made)
        return jnp.transpose(moments, (2, 0, 1, 3)), left, right

    return jax.shard_map(
        per_device,
        mesh=mesh,
        in_specs=(P(None, None, None, "gx", "gy"), P(None, "gx", "gy"), P(None, "gx", "gy")),
        out_specs=(
            P(None, None, None, "gx"),
            P(None, None, None, "gx", "gy"),
            P(None, None, None, "gx", "gy"),
        ),
        check_vma=False,
    )
```

```python
import functools
import jax
import jax.numpy as jnp
from jax import lax
from jax.experimental import pallas as pl
from jax.experimental.pallas import tpu as pltpu
from jax.sharding import PartitionSpec as P

MOMENTS = 3
SCALE = 6.0
EDGE = 2
GROUP = 8
HALF = 64
LANES = 128
SUBS = 8
SLOTS = 5
GRANT = 32 * 1024 * 1024
MESH = pl.DeviceIdType.MESH
SIXTH = 1.0 / SCALE
HALF_SQUARE = 0.5 * SCALE * SCALE
BENT_INNER = (2.0, -1.0, -1.0, -1.0, -1.0)
BENT_WINDOW = (2.0, -1.0, -1.0, 2.0, -1.0)


def tile(t):
    return slice(t * LANES, (t + 1) * LANES)


def up(t):
    return pltpu.roll(t, 1, 0)


def down(t):
    return pltpu.roll(t, t.shape[0] - 1, 0)


def speed(terms):
    a0, a12, b0, b12 = terms
    return a0 - 0.5 * a12, 0.5 * b12 - b0


def energy(pair, terms, on, factor=None):
    a0, a12, b0, b12 = terms
    a, b = on[0] * pair[0] + (a0 + a12), on[1] * pair[1] + (b0 + b12)
    return (a, b) if factor is None else (a * factor, b * factor)


def add_products(sums, left, right):
    for n in range(MOMENTS):
        for m in range(MOMENTS):
            (p, q), (r, s) = left[n], right[m]
            sums[0][n][m] = sums[0][n][m] + (p * r + q * s)
            sums[1][n][m] = sums[1][n][m] + (p * s - q * r)


def rights_of(at):
    return [at[0], at[3], at[4]]


def masked(mask, at):
    return [[jnp.where(mask, item, 0.0) for item in at[n]] for n in range(MOMENTS)]


def each_sum():
    return [(p, n, m) for p in range(2) for n in range(MOMENTS) for m in range(MOMENTS)]


def kernel(
    gxn, gyn, vec, bonds, onsite, out_mom, lbuf, rbuf,
    x, xe, f, fw, fo, hw, gb, gw, cc, cs, ms, c_own, c_left, c_right, hf, cv, bw, lk, state, keep, acc, part_mom,
    load_sem, send_sem, recv_sem, msend_sem, mrecv_sem,
):
    vectors, _, _, rows, cols = vec.shape
    tall = c_own.shape[1]
    tiles = cols // LANES
    last = tiles - 1
    gx = lax.axis_index("gx")
    gy = lax.axis_index("gy")

    def peer(dx, dy):
        return (lax.rem(gx + dx + gxn, gxn), lax.rem(gy + dy + gyn, gyn))

    barrier = pltpu.get_barrier_semaphore()
    near = [(dx % gxn, dy % gyn) for dx in (-1, 1) for dy in (0, 1, -1)]
    near += [(0, dy) for dy in range(gyn)]
    near = [one for k, one in enumerate(near) if one != (0, 0) and one not in near[:k]]
    for dx, dy in near:
        pl.semaphore_signal(barrier, inc=1, device_id=peer(dx, dy), device_id_type=MESH)

    low, high = slice(0, EDGE), slice(SUBS - EDGE, SUBS)
    loads = [
        pltpu.make_async_copy(vec.at[:, :, :, 0:EDGE, :], xe.at[:, :, :, low, :], load_sem.at[0]),
        pltpu.make_async_copy(
            vec.at[:, :, :, rows - EDGE : rows, :], xe.at[:, :, :, high, :], load_sem.at[1]
        ),
        pltpu.make_async_copy(bonds, f.at[0:3], load_sem.at[2]),
        pltpu.make_async_copy(onsite, f.at[3:5], load_sem.at[3]),
        pltpu.make_async_copy(vec, x, load_sem.at[4]),
    ]
    for copy in loads:
        copy.start()

    hw[:, :, 0, 1 : SUBS - EDGE, :] = jnp.zeros((vectors, 2, SUBS - EDGE - 1, cols), jnp.float32)
    hw[:, :, 1, EDGE : SUBS - 1, :] = jnp.zeros((vectors, 2, SUBS - EDGE - 1, cols), jnp.float32)
    acc[...] = jnp.zeros_like(acc)
    sends = []

    def send(src, dst, dx, dy):
        n = len(sends)
        copy = pltpu.make_async_remote_copy(
            src_ref=src, dst_ref=dst, send_sem=send_sem.at[n], recv_sem=recv_sem.at[n],
            device_id=peer(dx, dy), device_id_type=MESH,
        )
        sends.append(copy)
        return copy

    def packed(items):
        count = items[0][0].shape[0]
        lane = lax.broadcasted_iota(jnp.int32, (count, LANES), 1)
        spot = lax.rem(lane, HALF)
        total = None
        for k, (first, final) in enumerate(items):
            both = jnp.where(lane < HALF, first, final)
            place = lax.rem(spot + (2 * LANES - GROUP * k - GROUP // 2), LANES)
            moved = jnp.take_along_axis(both, place, axis=1)
            total = jnp.where(spot // GROUP == k, moved, total) if k else moved
        return total

    def sides_of(four):
        lane = lax.broadcasted_iota(jnp.int32, four[0].shape, 1)
        start = lane + jnp.where(lane < HALF, 2, 4)
        spot = lax.rem(lane, GROUP)
        total = None
        for k, one in enumerate(four):
            moved = jnp.take_along_axis(one, lax.rem(start + (LANES - 2 * k), LANES), axis=1)
            total = jnp.where(spot // 2 == k, moved, total) if k else moved
        return total

    def ends(ref, *index):
        return ref[(*index, slice(None), slice(0, LANES))], ref[
            (*index, slice(None), slice(cols - LANES, cols))
        ]

    sub8 = lax.broadcasted_iota(jnp.int32, (SUBS, LANES), 0)
    lane8 = lax.broadcasted_iota(jnp.int32, (SUBS, LANES), 1)

    def window_a(t):
        return jnp.where(
            sub8 < 4, pltpu.roll(t[0:SUBS], 1, 0), pltpu.roll(t[rows - SUBS : rows], SUBS - 2, 0)
        )

    def window_b(t):
        return jnp.where(
            sub8 < 4, pltpu.roll(t[0:SUBS], 2, 0), pltpu.roll(t[rows - SUBS : rows], SUBS - 1, 0)
        )

    for copy in loads[:4]:
        copy.wait()
    for p in range(2):
        for sub in range(2):
            cc[2 * p + sub] = packed([ends(xe, v, p, sub) for v in range(vectors)])
    cs[0] = sides_of([cc[k] for k in range(4)])

    def rim_rows(t):
        return jnp.where(sub8 < 4, t[0:SUBS], t[rows - SUBS : rows])

    cc[4] = packed([tuple(rim_rows(t) for t in ends(f, k)) for k in range(5)])
    cs[1] = cc[4]
    lane_r = lax.broadcasted_iota(jnp.int32, (rows, LANES), 1)
    core = slice(0, rows)

    def pack_block():
        loads[4].wait()
        for p in range(2):
            for sub in range(2):
                c_own[2 * p + sub, core] = packed([ends(x, v, p, sub) for v in range(vectors)])
        c_own[4, core] = packed([ends(f, k) for k in range(5)])
        ms[0] = sides_of([c_own[k, core] for k in range(4)])
        ms[1] = c_own[4, core]

    def fill(g, bent, fields, t):
        for i, item in enumerate(fields):
            g[3, i, :, tile(t)] = item
            g[0, i, :, tile(t)] = item * SIXTH
            g[1, i, :, tile(t)] = item * (2.0 * SIXTH)
            if i < 5:
                g[2, i, :, tile(t)] = item * (bent[i] * SIXTH * SIXTH)

    def turned(items, shift):
        size = items[0].shape
        lane = lax.broadcasted_iota(jnp.int32, size, 1)
        rolled = [pltpu.roll(t, shift % LANES, 1) for t in items]
        if shift > 0:
            return rolled[:1] + [jnp.where(lane == 0, rolled[t - 1], rolled[t]) for t in range(1, tiles)]
        return [
            jnp.where(lane == LANES - 1, rolled[t + 1], rolled[t]) for t in range(last)
        ] + rolled[last:]

    def inner_terms(a, b, w):
        left, right = turned(b, 1), turned(a, -1)
        found = []
        for t in range(tiles):
            f0, f1, f2, d1, d2 = (gb[w, i, :, tile(t)] for i in range(5))
            found.append((f0 * b[t], f1 * up(b[t]) + f2 * left[t], f0 * a[t], d1 * down(a[t]) + d2 * right[t]))
        return found

    def window_terms(a, b, w, leak=None):
        b_up, a_down = [down(t) for t in b], [up(t) for t in a]
        left, right = turned(b_up, 1), turned(a_down, -1)
        found = []
        for t in range(tiles):
            f0, f1, f2, d0, d2 = (gw[w, i, :, tile(t)] for i in range(5))
            over_a = a[t] if leak is None else a[t] + leak[0][t]
            over_b = b[t] if leak is None else b[t] + leak[1][t]
            found.append((f0 * b_up[t], f1 * over_b + f2 * left[t], d0 * a_down[t], f1 * over_a + d2 * right[t]))
        return found

    def both(items):
        return [item[0] for item in items], [item[1] for item in items]

    def at_tile(pair, t):
        return pair[0][t], pair[1][t]

    def chains(q0, terms, g, leaks):
        def on(w, t):
            return g[w, 5, :, tile(t)], g[w, 6, :, tile(t)]

        def less(pair, other, times=None):
            return both(
                [
                    tuple(
                        one - (two if times is None else two * times)
                        for one, two in zip(at_tile(pair, t), at_tile(other, t))
                    )
                    for t in range(tiles)
                ]
            )

        def stepped(pair, found, w):
            return both([energy(at_tile(pair, t), found[t], on(w, t)) for t in range(tiles)])

        t0 = terms(*q0, 3, *leaks[0:1])
        m0 = both([speed(item) for item in t0])
        q1 = stepped(q0, t0, 3)
        t1 = terms(*q1, 3, *leaks[1:2])
        n1 = both([speed(item) for item in t1])
        q2 = less(stepped(q1, t1, 3), q0, HALF_SQUARE)
        n2 = both([(a0 + a12, -(b0 + b12)) for a0, a12, b0, b12 in terms(*q2, 2)])
        m1 = stepped(m0, terms(*m0, 0, *leaks[2:3]), 0)
        m2 = less(stepped(m1, terms(*m1, 1), 1), m0)
        return q1, (m0, m1, m2, n1, n2)

    def inside_lanes(t):
        keep_lanes = None
        if t == 0:
            keep_lanes = lane8 >= EDGE
        if t == last:
            end = lane8 < LANES - EDGE
            keep_lanes = end if keep_lanes is None else keep_lanes & end
        return keep_lanes

    def inside(sub, r, t):
        keep_cells = inside_lanes(t)
        cuts = []
        if r == 0:
            cuts.append(sub8 >= EDGE - sub)
        if r == rows - SUBS:
            cuts.append(sub8 < SUBS - 1 - sub)
        for one in cuts:
            keep_cells = one if keep_cells is None else keep_cells & one
        return keep_cells

    def one_vector(v, carry):
        for p in range(2):
            q0 = tuple([x[v, p, sub, :, tile(t)] for t in range(tiles)] for sub in range(2))
            q1, slots = chains(q0, inner_terms, gb, ())
            for s, pair in enumerate(slots):
                for t in range(tiles):
                    for sub in range(2):
                        keep[s, p, sub, :, tile(t)] = pair[sub][t]
                    a, b = pair[0][t], pair[1][t]
                    ends_a, ends_b = (a[0:SUBS], a[rows - SUBS : rows]), (b[0:SUBS], b[rows - SUBS : rows])
                    over = jnp.where(sub8 == 3, pltpu.roll(ends_b[0], 3, 0), ends_b[1])
                    over = jnp.where(sub8 == 5, pltpu.roll(ends_a[1], SUBS - 2, 0), over)
                    bw[v, p, s, :, tile(t)] = jnp.where(
                        (sub8 == 1) | (sub8 == 2), pltpu.roll(ends_a[0], 1, 0), over
                    )
            for s, pair in enumerate((q0, q1, slots[0])):
                for t in range(tiles):
                    lk[v, p, s, 0, :, tile(t)] = jnp.where(sub8 == 1, window_a(pair[0][t]), 0.0)
                    lk[v, p, s, 1, :, tile(t)] = jnp.where(sub8 == 6, window_b(pair[1][t]), 0.0)
            for buf, pair in ((lbuf, slots[2]), (rbuf, slots[4])):
                for sub in range(2):
                    for t in range(tiles):
                        value = -pair[sub][t] if p == 0 else pair[sub][t]
                        buf[v, 1 - p, sub, :, tile(t)] = value.astype(jnp.bfloat16)

        for r in range(0, rows, SUBS):
            band = slice(r, r + SUBS)
            sums = [[[acc[p, n, m, band, :] for m in range(MOMENTS)] for n in range(MOMENTS)] for p in range(2)]
            for sub in range(2):
                for t in range(tiles):
                    at = [[keep[s, p, sub, band, tile(t)] for p in range(2)] for s in range(SLOTS)]
                    mask = inside(sub, r, t)
                    add_products(sums, at[:MOMENTS] if mask is None else masked(mask, at), rights_of(at))
            for p, n, m in each_sum():
                acc[p, n, m, band, :] = sums[p][n][m]
        return carry

    def own_block():
        sub_r = lax.broadcasted_iota(jnp.int32, (rows, LANES), 0)
        shifted = turned([f[2, :, tile(t)] for t in range(tiles)], -1)
        for t in range(tiles):
            inner = jnp.where(sub_r == 0, 0.0, f[1, :, tile(t)])
            fill(
                gb,
                BENT_INNER,
                (f[0, :, tile(t)], inner, f[2, :, tile(t)], down(inner), shifted[t],
                 f[3, :, tile(t)], f[4, :, tile(t)]),
                t,
            )
            for k in range(4):
                fo[k, :, tile(t)] = window_a(f[k, :, tile(t)])
            fo[4, :, tile(t)] = window_b(f[4, :, tile(t)])
        lax.fori_loop(0, vectors, one_vector, 0)

    early = gx == 0

    @pl.when(early)
    def _():
        pack_block()
        own_block()

    pl.semaphore_wait(barrier, len(near))

    past, ahead = slice(rows, rows + EDGE), slice(tall - EDGE, tall)
    sides = [
        send(ms, c_right.at[:, core, :], 0, -1),
        send(ms, c_left.at[:, core, :], 0, 1),
    ]
    rims = [
        send(f.at[0:4, rows - 1 : rows, :], fw.at[0:4, 0:1, :], 1, 0),
        send(f.at[4:5, rows - 2 : rows, :], fw.at[4:5, 0:2, :], 1, 0),
    ]
    for src, dst, dy in ((cs, c_right, -1), (cs, c_left, 1), (cc, c_own, 0)):
        rims.append(send(src.at[:, high, :], dst.at[:, ahead, :], 1, dy))
    rims += [
        send(xe.at[:, :, 1, SUBS - 2 : SUBS, :], hw.at[:, :, 1, 0:2, :], 1, 0),
        send(xe.at[:, :, 0, SUBS - 1 : SUBS, :], hw.at[:, :, 0, 0:1, :], 1, 0),
        send(f.at[0:4, 0:2, :], fw.at[0:4, SUBS - 2 : SUBS, :], -1, 0),
        send(f.at[4:5, 0:1, :], fw.at[4:5, SUBS - 1 : SUBS, :], -1, 0),
    ]
    for src, dst, dy in ((cs, c_right, -1), (cs, c_left, 1), (cc, c_own, 0)):
        rims.append(send(src.at[:, low, :], dst.at[:, past, :], -1, dy))
    rims += [
        send(xe.at[:, :, 0, 0:2, :], hw.at[:, :, 0, SUBS - 2 : SUBS, :], -1, 0),
        send(xe.at[:, :, 1, 0:1, :], hw.at[:, :, 1, SUBS - 1 : SUBS, :], -1, 0),
    ]

    @pl.when(early)
    def _():
        for copy in sides:
            copy.start()

    for copy in rims:
        copy.start()

    @pl.when(jnp.logical_not(early))
    def _():
        pack_block()
        for copy in sides:
            copy.start()
        own_block()

    row_sends = rims[5:7] + rims[12:14]
    for copy in sides + rims[0:5] + rims[7:12]:
        copy.wait_recv()

    taken_a = (sub8 < 1) | (sub8 >= SUBS - 2)
    taken_b = (sub8 < 2) | (sub8 >= SUBS - 1)
    cut = (sub8 == 3) | (sub8 == SUBS - 1)
    windows = [
        [jnp.where(taken_b if k == 4 else taken_a, fw[k, :, tile(t)], fo[k, :, tile(t)]) for t in range(tiles)]
        for k in range(5)
    ]
    for k in (0, 2):
        windows[k] = [jnp.where(cut, 0.0, t) for t in windows[k]]
    far = turned([up(t) for t in windows[2]], -1)
    for t in range(tiles):
        fill(
            gw,
            BENT_WINDOW,
            (windows[0][t], windows[1][t], windows[2][t], up(windows[0][t]), far[t], windows[3][t], windows[4][t]),
            t,
        )


    tlane = lax.broadcasted_iota(jnp.int32, (tall, LANES), 1)
    tspot = lax.rem(tlane, GROUP)
    on_left = tlane < HALF
    from_side = jnp.where(on_left, tspot, tspot - 2) // 2 == 1
    side = jnp.where(on_left, c_left[0], c_right[0])
    side_start = tlane + jnp.where(on_left, LANES - 2, LANES - 4)

    def joined(k):
        moved = jnp.take_along_axis(side, lax.rem(side_start + 2 * k, LANES), axis=1)
        return jnp.where(from_side, moved, c_own[k])

    field_tile = jnp.where(from_side, jnp.where(on_left, c_left[1], c_right[1]), c_own[4])
    place = (tlane // HALF) * HALF + tspot
    for k in range(5):
        hf[k] = jnp.take_along_axis(field_tile, place + GROUP * k, axis=1)
    hf[5] = down(hf[1])
    hf[6] = jnp.take_along_axis(field_tile, lax.rem(place + (2 * GROUP + 1), LANES), axis=1)
    h_on = (hf[3], hf[4])

    def rim_terms(a, b):
        f0, f1, f2, d1, d2 = hf[0], hf[1], hf[2], hf[5], hf[6]
        return (
            f0 * b, f1 * up(b) + f2 * pltpu.roll(b, 1, 1),
            f0 * a, d1 * down(a) + d2 * pltpu.roll(a, LANES - 1, 1),
        )

    for p in range(2):
        q0 = (joined(2 * p), joined(2 * p + 1))
        t0 = rim_terms(*q0)
        m0 = speed(t0)
        q1 = energy(q0, t0, h_on)
        t1 = rim_terms(*q1)
        n1 = speed(t1)
        h1 = energy(q1, t1, h_on)
        q2 = (h1[0] - HALF_SQUARE * q0[0], h1[1] - HALF_SQUARE * q0[1])
        n2 = tuple(item / HALF_SQUARE for item in speed(rim_terms(*q2)))
        m1 = energy(m0, rim_terms(*m0), h_on, SIXTH)
        h2 = energy(m1, rim_terms(*m1), h_on, 2.0 * SIXTH)
        m2 = (h2[0] - m0[0], h2[1] - m0[1])
        for s, pair in enumerate((m0, m1, m2, n1, n2)):
            for sub in range(2):
                cv[s, p, sub] = pair[sub][0:rows]

    spot8 = lax.rem(lane8, GROUP)
    rim_lanes = ((lane8 < HALF) & ((spot8 == 4) | (spot8 == 5))) | (
        (lane8 >= HALF) & ((spot8 == 2) | (spot8 == 3))
    )


    def none():
        zero = jnp.zeros((SUBS, LANES), jnp.float32)
        return [[[zero for _ in range(MOMENTS)] for _ in range(MOMENTS)] for _ in range(2)]

    for r in range(0, rows, SUBS):
        band = slice(r, r + SUBS)
        sums = none()
        for sub in range(2):
            at = [[cv[s, p, sub, band] for p in range(2)] for s in range(SLOTS)]
            add_products(sums, masked(rim_lanes, at), rights_of(at))
        for p, n, m in each_sum():
            value = acc[p, n, m, band, :] + sums[p][n][m]
            acc[p, n, m, band, :] = value * SIXTH if m == 1 else value

    count = 2 * MOMENTS * MOMENTS * rows
    rest = acc[...].reshape(count, LANES)
    ones = jnp.ones((SUBS, LANES), jnp.bfloat16)
    total = None
    for _ in range(3):
        piece = rest.astype(jnp.bfloat16)
        rest = rest - piece.astype(jnp.float32)
        part = lax.dot_general(
            ones, piece, (((1,), (1,)), ((), ())), preferred_element_type=jnp.float32
        )
        total = part if total is None else total + part

    for copy in row_sends:
        copy.wait_recv()

    from_a = (sub8 == 1) | (sub8 == 2) | (sub8 == 5)
    planes = [(v, p) for v in range(vectors) for p in range(2)]

    def pair_of(ref, *index):
        return tuple([ref[(*index, sub, slice(None), tile(t))] for t in range(tiles)] for sub in range(2))

    def on_window(pair, found, w):
        return both(
            [
                energy(at_tile(pair, t), found[t], (gw[w, 5, :, tile(t)], gw[w, 6, :, tile(t)]))
                for t in range(tiles)
            ]
        )

    def put(k, v, p, pair):
        for sub in range(2):
            for t in range(tiles):
                state[k, v, p, sub, :, tile(t)] = pair[sub][t]

    def add(v, p, s, pair):
        for t in range(tiles):
            change = jnp.where(from_a, pair[0][t], up(pair[1][t]))
            bw[v, p, s, :, tile(t)] = bw[v, p, s, :, tile(t)] + change

    def minus(pair, other, times=None):
        return tuple(
            [one - (two if times is None else two * times) for one, two in zip(pair[sub], other[sub])]
            for sub in range(2)
        )

    for v, p in planes:
        pair = pair_of(hw, v, p)
        found = window_terms(*pair, 3, pair_of(lk, v, p, 0))
        m0 = both([speed(item) for item in found])
        put(0, v, p, on_window(pair, found, 3))
        put(1, v, p, m0)
        add(v, p, 0, m0)
    for v, p in planes:
        pair = pair_of(state, 0, v, p)
        found = window_terms(*pair, 3, pair_of(lk, v, p, 1))
        add(v, p, 3, both([speed(item) for item in found]))
        put(2, v, p, minus(on_window(pair, found, 3), pair_of(hw, v, p), HALF_SQUARE))
    for v, p in planes:
        pair = pair_of(state, 1, v, p)
        m1 = on_window(pair, window_terms(*pair, 0, pair_of(lk, v, p, 2)), 0)
        put(3, v, p, m1)
        add(v, p, 1, m1)
    for v, p in planes:
        found = window_terms(*pair_of(state, 2, v, p), 2)
        add(v, p, 4, both([(a0 + a12, -(b0 + b12)) for a0, a12, b0, b12 in found]))
    for v, p in planes:
        pair = pair_of(state, 3, v, p)
        add(v, p, 2, minus(on_window(pair, window_terms(*pair, 1), 1), pair_of(state, 1, v, p)))

    found = none()
    for t in range(tiles):
        sums = none()
        for v in range(vectors):
            at = [[bw[v, p, s, :, tile(t)] for p in range(2)] for s in range(SLOTS)]
            add_products(sums, at[:MOMENTS], rights_of(at))
        mask = inside_lanes(t)
        for p, n, m in each_sum():
            value = sums[p][n][m] if mask is None else jnp.where(mask, sums[p][n][m], 0.0)
            found[p][n][m] = value if t == 0 else found[p][n][m] + value
    row8 = jnp.where(sub8 < 4, jnp.where(sub8 == 2, 1, 0), jnp.where(sub8 == 6, rows - 2, rows - 1))
    row8 = jnp.where((sub8 == 0) | (sub8 == 4), -LANES, row8)
    per = LANES // rows
    for j in range(0, 2 * MOMENTS * MOMENTS, per):
        chosen = each_sum()[j : j + per]
        piece = jnp.zeros((SUBS, LANES), jnp.float32)
        for k, (p, n, m) in enumerate(chosen):
            value = jnp.sum(found[p][n][m], axis=1, keepdims=True)
            piece = jnp.where(lane8 == row8 + k * rows, value * SIXTH if m == 1 else value, piece)
        for step in (4, 2, 1):
            piece = piece + pltpu.roll(piece, step, 0)
        span = slice(j * rows, (j + len(chosen)) * rows)
        part_mom[0, :, span] = total[:, span] + piece[:, 0 : len(chosen) * rows]

    swaps = []
    for d in range(1, gyn):
        copy = pltpu.make_async_remote_copy(
            src_ref=part_mom.at[0, 0:1], dst_ref=part_mom.at[d, 0:1],
            send_sem=msend_sem.at[d - 1], recv_sem=mrecv_sem.at[d - 1],
            device_id=peer(0, d), device_id_type=MESH,
        )
        copy.start()
        swaps.append(copy)

    def patch(v, carry):
        turn_first = lax.rem(2 * LANES - GROUP // 2 - GROUP * v, LANES)
        turn_last = lax.rem(2 * LANES - GROUP // 2 + HALF - GROUP * v, LANES)
        for p in range(2):
            for sub in range(2):
                for s, buf in ((2, lbuf), (4, rbuf)):
                    side = cv[s, p, sub]
                    for t in range(tiles):
                        value = buf[v, 1 - p, sub, :, tile(t)].astype(jnp.float32)
                        over = bw[v, p, s, :, tile(t)]
                        edge = -side if p == 0 else side
                        over = -over if p == 0 else over
                        top = jnp.where(
                            sub8 < EDGE - sub, pltpu.roll(over, SUBS - 1 - 2 * sub, 0), value[0:SUBS]
                        )
                        bottom = jnp.where(
                            sub8 >= SUBS - 1 - sub, over if sub else pltpu.roll(over, 2, 0), value[rows - SUBS : rows]
                        )
                        value = jnp.concatenate([top, value[SUBS : rows - SUBS], bottom] if rows > 2 * SUBS else [top, bottom], 0)
                        if t == 0:
                            value = jnp.where(lane_r < EDGE, pltpu.roll(edge, turn_first, 1), value)
                        if t == last:
                            value = jnp.where(lane_r >= LANES - EDGE, pltpu.roll(edge, turn_last, 1), value)
                        buf[v, 1 - p, sub, :, tile(t)] = value.astype(jnp.bfloat16)
        return carry

    lax.fori_loop(0, vectors, patch, 0)

    for copy in sends + swaps:
        copy.wait_send()
    for copy in swaps:
        copy.wait_recv()
    total = part_mom[0]
    for d in range(1, gyn):
        total = total + part_mom[d]
    out_mom[...] = total / float(vectors * cols * gyn)


def writer(total, lbuf, rbuf, out_mom, out_left, out_right, mom, out_sem):
    outs = [
        pltpu.make_async_copy(lbuf, out_left, out_sem.at[0]),
        pltpu.make_async_copy(rbuf, out_right, out_sem.at[1]),
    ]
    for copy in outs:
        copy.start()
    rows = mom.shape[3]
    for p in range(2):
        for n in range(MOMENTS):
            for m in range(MOMENTS):
                k = (p * MOMENTS + n) * MOMENTS + m
                mom[n, m, p : p + 1, :] = total[0:1, k * rows : (k + 1) * rows]
    outs.append(pltpu.make_async_copy(mom, out_mom, out_sem.at[2]))
    outs[2].start()
    for copy in outs:
        copy.wait()


def solution(mesh):
    gxn, gyn = mesh.shape["gx"], mesh.shape["gy"]

    def per_device(vectors, bonds, onsite):
        count, _, _, rows, cols = vectors.shape
        tall = rows + 8
        f32 = jnp.float32
        in_hbm = pl.BlockSpec(memory_space=pltpu.HBM)
        last = jax.ShapeDtypeStruct(vectors.shape, jnp.bfloat16)
        sends = 16
        in_vmem = pl.BlockSpec(memory_space=pltpu.VMEM)
        sums = (8, 2 * MOMENTS * MOMENTS * rows)
        made = pl.pallas_call(
            functools.partial(kernel, gxn, gyn),
            out_shape=(
                pltpu.VMEM(sums, f32),
                pltpu.VMEM(vectors.shape, jnp.bfloat16),
                pltpu.VMEM(vectors.shape, jnp.bfloat16),
            ),
            in_specs=[in_hbm] * 3,
            out_specs=(in_vmem,) * 3,
            scratch_shapes=[
                pltpu.VMEM(vectors.shape, f32),
                pltpu.VMEM((count, 2, 2, SUBS, cols), f32),
                pltpu.VMEM((5, rows, cols), f32),
                pltpu.VMEM((5, SUBS, cols), f32),
                pltpu.VMEM((5, SUBS, cols), f32),
                pltpu.VMEM((count, 2, 2, SUBS, cols), f32),
                pltpu.VMEM((4, 7, rows, cols), f32),
                pltpu.VMEM((4, 7, SUBS, cols), f32),
                pltpu.VMEM((5, SUBS, LANES), f32),
                pltpu.VMEM((2, SUBS, LANES), f32),
                pltpu.VMEM((2, rows, LANES), f32),
                pltpu.VMEM((5, tall, LANES), f32),
                pltpu.VMEM((2, tall, LANES), f32),
                pltpu.VMEM((2, tall, LANES), f32),
                pltpu.VMEM((7, tall, LANES), f32),
                pltpu.VMEM((SLOTS, 2, 2, rows, LANES), f32),
                pltpu.VMEM((count, 2, SLOTS, SUBS, cols), f32),
                pltpu.VMEM((count, 2, 3, 2, SUBS, cols), f32),
                pltpu.VMEM((4, count, 2, 2, SUBS, cols), f32),
                pltpu.VMEM((SLOTS, 2, 2, rows, cols), f32),
                pltpu.VMEM((2, MOMENTS, MOMENTS, rows, LANES), f32),
                pltpu.VMEM((gyn, *sums), f32),
                pltpu.SemaphoreType.DMA((5,)),
                pltpu.SemaphoreType.DMA((sends,)),
                pltpu.SemaphoreType.DMA((sends,)),
                pltpu.SemaphoreType.DMA((gyn - 1,)),
                pltpu.SemaphoreType.DMA((gyn - 1,)),
            ],
            compiler_params=pltpu.CompilerParams(
                collective_id=0, has_side_effects=True, vmem_limit_bytes=GRANT
            ),
        )(*(pltpu.with_memory_space_constraint(array, pltpu.HBM) for array in (vectors, bonds, onsite)))
        made = [pltpu.with_memory_space_constraint(array, pltpu.VMEM) for array in made]
        moments, left, right = pl.pallas_call(
            writer,
            out_shape=(
                jax.ShapeDtypeStruct((MOMENTS, MOMENTS, 2, rows), f32), last, last,
            ),
            in_specs=[in_vmem] * 3,
            out_specs=(in_hbm,) * 3,
            scratch_shapes=[
                pltpu.VMEM((MOMENTS, MOMENTS, 2, rows), f32),
                pltpu.SemaphoreType.DMA((3,)),
            ],
            compiler_params=pltpu.CompilerParams(vmem_limit_bytes=GRANT),
        )(*made)
        return jnp.transpose(moments, (2, 0, 1, 3)), left, right

    return jax.shard_map(
        per_device,
        mesh=mesh,
        in_specs=(P(None, None, None, "gx", "gy"), P(None, "gx", "gy"), P(None, "gx", "gy")),
        out_specs=(
            P(None, None, None, "gx"),
            P(None, None, None, "gx", "gy"),
            P(None, None, None, "gx", "gy"),
        ),
        check_vma=False,
    )
```
